8 devices in a mesh: dp: 2 (over z, y), cp: 4 (over x, core).
Axes of the slice: x: 2, y: 2, z: 1, core: 2. Of those that a mesh axis runs over, the one named last changes fastest.
Arguments:
- x: bfloat16 [128, 2560], P('dp'), parts along dimension 0
- w_dq: bfloat16 [2560, 768], replicated
- g_q: float32 [768], replicated
- w_uq: bfloat16 [768, 3840], replicated
- w_dkv: bfloat16 [2560, 288], replicated
- g_kv: float32 [256], replicated
- w_uk: bfloat16 [256, 40, 64], replicated
- w_uv: bfloat16 [256, 40, 64], replicated
- w_o: bfloat16 [2560, 2560], replicated
- cache_c: bfloat16 [128, 16384, 256], P('dp', 'cp'), parts along dimension 0
- cache_kr: bfloat16 [128, 16384, 32], P('dp', 'cp'), parts along dimension 0
- ctx_len: int32 [128], P('dp'), parts along dimension 0
Outputs:
- output 1: bfloat16 [128, 2560], P('dp'), parts along dimension 0
- output 2: bfloat16 [128, 256], P('dp'), parts along dimension 0
- output 3: bfloat16 [128, 32], P('dp'), parts along dimension 0
There are 2 independent parts. The reference program is written for one: setup_inputs(seed, part) draws one part's arguments, and reference() takes and returns one part's arrays. A program takes and returns all parts, laid end to end along the dimension named above; an argument that names none is the same for every part.
All inputs are finite; a program needn't handle non-finite values.
Results may differ from the reference program's by a relative error of at most 0.00630591.
Values sent between devices are 32-bit elements.
A program may use at most 1 GiB of HBM per device.

```python
import jax
import jax.numpy as jnp
from jax import lax

BATCH = 64
T_DEV = 4096
GROUP_SIZE = 4
D_MODEL = 2560
HEADS = 40
Q_LORA = 768
LATENT = 256
NOPE_DIM = 64
ROPE_DIM = 32
V_DIM = 64

SEQ = T_DEV * GROUP_SIZE
QK_DIM = NOPE_DIM + ROPE_DIM
NORM_EPS = 1e-6
ROPE_THETA = 10000.0


def rms_norm(values, gain_vec):
    mean_sq = jnp.mean(jnp.square(values), axis=-1, keepdims=True)
    return values * lax.rsqrt(mean_sq + NORM_EPS) * gain_vec


def rope_tables(positions):
    half_dim = ROPE_DIM // 2
    inv_freq = ROPE_THETA ** (-2.0 * jnp.arange(half_dim, dtype=jnp.float32) / ROPE_DIM)
    angles = positions.astype(jnp.float32)[..., None] * inv_freq
    return jnp.cos(angles), jnp.sin(angles)


def rope_rotate(values, cos_tab, sin_tab):
    half_dim = values.shape[-1] // 2
    lo_half = values[..., :half_dim]
    hi_half = values[..., half_dim:]
    return jnp.concatenate([lo_half * cos_tab - hi_half * sin_tab, hi_half * cos_tab + lo_half * sin_tab], axis=-1)


def setup_inputs(seed: int = 0, part: int = 0) -> dict:
    shared_keys = jax.random.split(jax.random.key(seed), 8)
    part_keys = jax.random.split(jax.random.fold_in(jax.random.key(seed + 1), part), 8)

    def draw_normal(key, shape, std):
        return jax.random.normal(key, shape, jnp.float32) * std

    x = draw_normal(part_keys[0], (BATCH, D_MODEL), 1.0).astype(jnp.bfloat16)
    w_dq = draw_normal(shared_keys[0], (D_MODEL, Q_LORA), D_MODEL ** -0.5).astype(jnp.bfloat16)
    g_q = jax.random.uniform(shared_keys[1], (Q_LORA,), jnp.float32, 0.5, 1.5)
    w_uq = draw_normal(shared_keys[2], (Q_LORA, HEADS * QK_DIM), Q_LORA ** -0.5).astype(jnp.bfloat16)
    w_dkv = draw_normal(shared_keys[3], (D_MODEL, LATENT + ROPE_DIM), D_MODEL ** -0.5).astype(jnp.bfloat16)
    g_kv = jax.random.uniform(shared_keys[4], (LATENT,), jnp.float32, 0.5, 1.5)
    w_uk = draw_normal(shared_keys[5], (LATENT, HEADS, NOPE_DIM), LATENT ** -0.5).astype(jnp.bfloat16)
    w_uv = draw_normal(shared_keys[6], (LATENT, HEADS, V_DIM), LATENT ** -0.5).astype(jnp.bfloat16)
    w_o = draw_normal(shared_keys[7], (HEADS * V_DIM, D_MODEL), (HEADS * V_DIM) ** -0.5).astype(jnp.bfloat16)
    pos_ramp = 2.0 * jnp.arange(SEQ, dtype=jnp.float32) / SEQ - 1.0
    drift_dir = draw_normal(part_keys[1], (BATCH, 1, LATENT), 1.0)
    cache_c = (draw_normal(part_keys[2], (BATCH, SEQ, LATENT), 1.0) + drift_dir * pos_ramp[None, :, None]).astype(jnp.bfloat16)
    key_base = jnp.broadcast_to(draw_normal(part_keys[3], (BATCH, 1, ROPE_DIM), 1.0), (BATCH, SEQ, ROPE_DIM))
    cos_tab, sin_tab = rope_tables(jnp.arange(SEQ))
    cache_kr = (rope_rotate(key_base, cos_tab[None], sin_tab[None]) + draw_normal(part_keys[4], (BATCH, SEQ, ROPE_DIM), 0.5)).astype(jnp.bfloat16)
    ctx_len = jax.random.randint(part_keys[5], (BATCH,), SEQ // 2, SEQ, dtype=jnp.int32).at[0].set(SEQ - 1)
    return {'x': x, 'w_dq': w_dq, 'g_q': g_q, 'w_uq': w_uq, 'w_dkv': w_dkv, 'g_kv': g_kv, 'w_uk': w_uk, 'w_uv': w_uv, 'w_o': w_o, 'cache_c': cache_c, 'cache_kr': cache_kr, 'ctx_len': ctx_len}


def reference(x, w_dq, g_q, w_uq, w_dkv, g_kv, w_uk, w_uv, w_o, cache_c, cache_kr, ctx_len):
    cq_low = jnp.dot(x, w_dq, preferred_element_type=jnp.float32).astype(jnp.bfloat16)
    cq_norm = rms_norm(cq_low.astype(jnp.float32), g_q).astype(jnp.bfloat16)
    q_full = jnp.dot(cq_norm, w_uq, preferred_element_type=jnp.float32).astype(jnp.bfloat16).reshape(BATCH, HEADS, QK_DIM)
    cos_tab, sin_tab = rope_tables(ctx_len)
    q_rope = rope_rotate(q_full[:, :, NOPE_DIM:].astype(jnp.float32), cos_tab[:, None, :], sin_tab[:, None, :]).astype(jnp.bfloat16)
    q_lat = jnp.einsum('bhn,khn->bhk', q_full[:, :, :NOPE_DIM].astype(jnp.float32), w_uk.astype(jnp.float32)).astype(jnp.bfloat16)
    kv_full = jnp.dot(x, w_dkv, preferred_element_type=jnp.float32)
    c_new = rms_norm(kv_full[:, :LATENT], g_kv).astype(jnp.bfloat16)
    kr_new = rope_rotate(kv_full[:, LATENT:], cos_tab, sin_tab).astype(jnp.bfloat16)
    score_scale = QK_DIM ** -0.5
    positions = jnp.arange(SEQ)

    def attend_one(item_args):
        q_lat_r, q_rope_r, c_rows, kr_rows, c_new_r, kr_new_r, req_len = item_args
        scores = (jnp.dot(q_lat_r, c_rows.T, preferred_element_type=jnp.float32) + jnp.dot(q_rope_r, kr_rows.T, preferred_element_type=jnp.float32)) * score_scale
        scores = jnp.where(positions[None, :] < req_len, scores, -jnp.inf)
        new_score = (jnp.dot(q_lat_r, c_new_r, preferred_element_type=jnp.float32) + jnp.dot(q_rope_r, kr_new_r, preferred_element_type=jnp.float32)) * score_scale
        row_max = jnp.maximum(jnp.max(scores, axis=1), new_score)
        weights = jnp.exp(scores - row_max[:, None])
        new_weight = jnp.exp(new_score - row_max)
        row_sum = jnp.sum(weights, axis=1) + new_weight
        lat_acc = jnp.dot(weights.astype(jnp.bfloat16), c_rows, preferred_element_type=jnp.float32)
        lat_acc = lat_acc + new_weight.astype(jnp.bfloat16).astype(jnp.float32)[:, None] * c_new_r.astype(jnp.float32)[None, :]
        return lat_acc / row_sum[:, None]

    o_lat = lax.map(attend_one, (q_lat, q_rope, cache_c, cache_kr, c_new, kr_new, ctx_len)).astype(jnp.bfloat16)
    o_heads = jnp.einsum('bhk,khv->bhv', o_lat.astype(jnp.float32), w_uv.astype(jnp.float32)).astype(jnp.bfloat16)
    attn_out = jnp.dot(o_heads.reshape(BATCH, HEADS * V_DIM), w_o, preferred_element_type=jnp.float32)
    x_out = (x.astype(jnp.float32) + attn_out).astype(jnp.bfloat16)
    return x_out, c_new, kr_new
```

```python
import functools

import jax
import jax.numpy as jnp
import numpy as np
from jax import lax
from jax.experimental import pallas as pl
from jax.experimental.pallas import tpu as pltpu
from jax.sharding import PartitionSpec as P

F32, BF16 = jnp.float32, jnp.bfloat16
NORM_EPS = 1e-6
SCALE = np.float32(96 ** -0.5 * np.log2(np.e))
MASKED = -2.0e38
FLOOR = -1.0e38

NREQ, T, H, L, R, D, QL = 64, 4096, 40, 256, 32, 2560, 768
HP = 48
NT = 8
NB = 8
NOWN = NREQ // 2
LEAD = 3
NCT = 8
XPOSE_TILES = ((1, 0), (0, 0))


def decode_kernel(x_ref, gq_ref, gkv_ref, freq_ref, ctxv_ref, ctx_ref, wdq_h, wuq_h, wdkv_h, wuk_h, wuv_h, wo_h, c_h, kr_h,
                  xo_ref, co_ref, ko_ref,
                  wdq, wuq, wdkv, wuk, wuv, wo, cbuf, krbuf, qf, qrf, qb, qrb, cnf, krf,
                  sbuf, mbuf, ctb, send_a, recv_1, own_b, send_b, recv_2, ola, olb, xbuf,
                  wsem, csem, ksem, sa_sem, r1_sem, sb_sem, r2_sem, xs_sem, xr_sem):
    cp = lax.axis_index('cp')
    core = lax.rem(cp, 2)
    sibling = cp + 1 - 2 * core
    mirror = lax.rem(cp + 2, 4)

    barrier = pltpu.get_barrier_semaphore()
    for other in (sibling, mirror):
        pl.semaphore_signal(barrier, inc=1, device_id={'cp': other}, device_id_type=pl.DeviceIdType.MESH)

    weights = [pltpu.make_async_copy(h, v, wsem.at[k]) for k, (h, v) in enumerate(
        ((wdq_h, wdq), (wdkv_h, wdkv), (wuq_h, wuq), (wuk_h, wuk), (wuv_h, wuv), (wo_h, wo)))]

    def request(s):
        u = lax.rem(s, 2)
        half = (1 - core) * (1 - u) + core * u
        return half * NOWN + s // 2

    def cache_copies(s):
        b, slot = request(s), lax.rem(s, NB)
        return (pltpu.make_async_copy(c_h.at[b], cbuf.at[slot], csem.at[slot]),
                pltpu.make_async_copy(kr_h.at[b], krbuf.at[slot], ksem.at[slot]))

    def start(s):
        for copy in cache_copies(s):
            copy.start()

    def wait(s):
        for copy in cache_copies(s):
            copy.wait()

    for copy in weights[:4]:
        copy.start()
    for s in range(NB):
        start(s)

    lane128 = lax.broadcasted_iota(jnp.int32, (1, 128), 1)
    lane256 = lax.broadcasted_iota(jnp.int32, (1, 256), 1)

    dot = functools.partial(jnp.dot, preferred_element_type=F32)
    dot_t = functools.partial(lax.dot_general, dimension_numbers=(((1,), (1,)), ((), ())), preferred_element_type=F32)

    angle = ctxv_ref[...].astype(F32) * freq_ref[...]
    cos_t = jnp.cos(angle)
    sin_t = jnp.sin(angle) * jnp.where(lax.rem(lane128, 32) < 16, -1.0, 1.0)

    weights[0].wait()
    cq = [dot(x_ref[...], wdq[:, n * 256:(n + 1) * 256]).astype(BF16).astype(F32) for n in range(3)]
    mean_sq = sum(jnp.sum(v * v, axis=1, keepdims=True) for v in cq) * np.float32(1.0 / QL)
    inv_q = lax.rsqrt(mean_sq + NORM_EPS)
    cn = jnp.concatenate([(cq[n] * inv_q * gq_ref[:, n * 256:(n + 1) * 256]).astype(BF16) for n in range(3)], axis=1)

    weights[1].wait()
    kv = dot_t(x_ref[...], wdkv[:L, :])
    inv_kv = lax.rsqrt(jnp.sum(kv * kv, axis=1, keepdims=True) * np.float32(1.0 / L) + NORM_EPS)
    c_new = (kv * inv_kv * gkv_ref[...]).astype(BF16)
    co_ref[...] = c_new
    cnf[...] = c_new.astype(F32)
    kr = dot_t(x_ref[...], wdkv[L:L + R, :])
    kr = jnp.concatenate([kr, jnp.zeros((NREQ, 128 - R), F32)], axis=1)
    partner = jnp.where(lane128 < 16, pltpu.roll(kr, 112, 1), pltpu.roll(kr, 16, 1))
    kr_new = (kr * cos_t + partner * sin_t).astype(BF16)
    ko_ref[...] = kr_new[:, :R]
    krf[...] = jnp.where(lane128 < R, kr_new.astype(F32), 0.0)

    weights[2].wait()
    for n in range(15):
        qf[:, n * 256:(n + 1) * 256] = dot(cn, wuq[:, n * 256:(n + 1) * 256]).astype(BF16)

    row = lax.broadcasted_iota(jnp.int32, (256, 256), 0)
    col = lax.broadcasted_iota(jnp.int32, (256, 256), 1)
    src = lax.rem(col + jnp.where(col < 128, 0, 16), 32)
    for o in range(8):
        pick = jnp.where(row == src + 32 * o, 1.0, 0.0).astype(BF16)
        heads = [h for h in range(H) if ((96 * h + 64) % 256) // 32 == o]
        wins = [(96 * h + 64) // 256 for h in heads]
        both = dot(jnp.concatenate([qf[:, w * 256:(w + 1) * 256] for w in wins], axis=0), pick)
        for k, h in enumerate(heads):
            part = both[k * NREQ:(k + 1) * NREQ]
            qrf[pl.ds(h, NREQ, stride=H), :] = (part[:, :128] * cos_t + part[:, 128:] * sin_t).astype(BF16).astype(F32)

    weights[3].wait()
    nope = {h: (96 * h, 96 * h + 64) for h in range(H)}
    carry = {}
    for w in range(15):
        lo, hi = 256 * w, 256 * (w + 1)
        here = [(h, max(a, lo), min(b, hi)) for h, (a, b) in nope.items() if a < hi and b > lo]
        pieces, at = [], lo
        for h, a, b in here:
            if a > at:
                pieces.append(jnp.zeros((a - at, 256), BF16))
            pieces.append(wuk[h, a - nope[h][0]:b - nope[h][0], :])
            at = b
        if at < hi:
            pieces.append(jnp.zeros((hi - at, 256), BF16))
        window = qf[:, lo:hi]
        lhs = [window * jnp.where((lane256 >= a - lo) & (lane256 < b - lo), 1.0, 0.0).astype(BF16) for _, a, b in here]
        lat = dot(jnp.concatenate(lhs, axis=0), jnp.concatenate(pieces, axis=0))
        for k, (h, a, b) in enumerate(here):
            v = lat[k * NREQ:(k + 1) * NREQ]
            if a > nope[h][0]:
                v = v + carry.pop(h)
            if b < nope[h][1]:
                carry[h] = v
                continue
            v = v.astype(BF16).astype(F32)
            ola[pl.ds(h, NREQ, stride=H), :] = v[:, :128]
            olb[pl.ds(h, NREQ, stride=H), :] = v[:, 128:]
    pl.semaphore_wait(barrier, 2)

    def to_bf16(b, _):
        rows = pl.ds(pl.multiple_of(b * H, 8), H)
        qb[b] = jnp.concatenate([jnp.concatenate([ola[rows, :], olb[rows, :]], axis=1), jnp.zeros((HP - H, L), F32)], axis=0).astype(BF16)
        qrb[b] = jnp.concatenate([qrf[rows, :], jnp.zeros((HP - H, 128), F32)], axis=0).astype(BF16)
        return 0
    lax.fori_loop(0, NREQ, to_bf16, 0)

    def rcopy_1(i):
        return pltpu.make_async_remote_copy(src_ref=send_a.at[i], dst_ref=recv_1.at[i], send_sem=sa_sem.at[i], recv_sem=r1_sem.at[i],
                                            device_id={'cp': sibling}, device_id_type=pl.DeviceIdType.MESH)

    def rcopy_2(i):
        return pltpu.make_async_remote_copy(src_ref=send_b.at[i], dst_ref=recv_2.at[i], send_sem=sb_sem.at[i], recv_sem=r2_sem.at[i],
                                            device_id={'cp': mirror}, device_id_type=pl.DeviceIdType.MESH)

    def put_partial(ref, i, lo, hi, m, l):
        ref[i, 0:H, :] = lo
        ref[i, H:2 * H, :] = hi
        ml = jnp.zeros((8, 128), F32)
        for g in range(5):
            ml = jnp.where(lane128 == g, m[8 * g:8 * g + 8], ml)
            ml = jnp.where(lane128 == 8 + g, l[8 * g:8 * g + 8], ml)
        ref[i, 2 * H:2 * H + 8, :] = ml

    def get_partial(ref, i):
        ml = ref[i, 2 * H:2 * H + 8, :]
        spread = lambda at: jnp.concatenate([jnp.broadcast_to(ml[:, at + g:at + g + 1], (8, 128)) for g in range(5)], axis=0)
        return ref[i, 0:H, :], ref[i, H:2 * H, :], spread(0), spread(8)

    def combine_1(i):
        lo_p, hi_p, m_p, l_p = get_partial(own_b, i)
        lo_q, hi_q, m_q, l_q = get_partial(recv_1, i)
        m = jnp.maximum(m_p, m_q)
        f_p, f_q = jnp.exp2(m_p - m), jnp.exp2(m_q - m)
        put_partial(send_b, i, lo_p * f_p + lo_q * f_q, hi_p * f_p + hi_q * f_q, m, l_p * f_p + l_q * f_q)

    def combine_2(i):
        lo_p, hi_p, m_p, l_p = get_partial(send_b, i)
        lo_q, hi_q, m_q, l_q = get_partial(recv_2, i)
        ii = jnp.minimum(i, NOWN - 1)
        b = core * NOWN + ii
        c_row, k_row = cnf[pl.ds(b, 1), :], krf[pl.ds(b, 1), :]
        q, qr = qb[b].astype(F32)[:H], qrb[b].astype(F32)[:H]
        part = q[:, :128] * c_row[:, :128] + q[:, 128:] * c_row[:, 128:] + qr * k_row
        s_new = jnp.broadcast_to(jnp.sum(part, axis=1, keepdims=True) * SCALE, (H, 128))
        m = jnp.maximum(jnp.maximum(m_p, m_q), s_new)
        f_p, f_q, w_new = jnp.exp2(m_p - m), jnp.exp2(m_q - m), jnp.exp2(s_new - m)
        inv = 1.0 / (l_p * f_p + l_q * f_q + w_new)
        w_new = w_new.astype(BF16).astype(F32)
        rows = pl.ds(pl.multiple_of(i * H, 8), H)
        ola[rows, :] = (lo_p * f_p + lo_q * f_q + w_new * c_row[:, :128]) * inv
        olb[rows, :] = (hi_p * f_p + hi_q * f_q + w_new * c_row[:, 128:]) * inv

    def attend():
        count = [0]

        def qk_tile(s, par, j, mx):
            slot, b = lax.rem(s, NB), request(s)
            n = ctx_ref[b] - cp * T
            at = pl.ds(256 * j, 256)
            c = cbuf[slot, at, :]
            if (par, j // 2) in XPOSE_TILES:
                v = dot_t(qb[b], c)
            else:
                t = count[0] % NCT
                count[0] += 1
                ctb[t] = c.T
                v = dot(qb[b], ctb[t])
            v = (v + dot(qrb[b][:, :R], krbuf[slot, :, at]))[:H]
            v = jnp.where(lane256 + j * 256 < n, v, MASKED)
            sbuf[par, :, at] = v
            for k in range(2):
                part = v[:, k * 128:(k + 1) * 128]
                mx = part if mx is None else jnp.maximum(mx, part)
            return mx

        def pv_tile(s, par, j, mk, st):
            ws = []
            for k in range(2):
                w = jnp.exp2(sbuf[par, :, pl.ds(j * 256 + k * 128, 128)] * SCALE - mk)
                st['l'] = w if st['l'] is None else st['l'] + w
                ws.append(w)
            w = jnp.concatenate([jnp.concatenate(ws, axis=1), jnp.zeros((HP - H, 256), F32)], axis=0).astype(BF16)
            p = dot(w, cbuf[lax.rem(s, NB), pl.ds(256 * j, 256), :])
            st[j % 2] = p if st[j % 2] is None else st[j % 2] + p

        def half(s, par, out, out_i, last=False):
            mk = jnp.broadcast_to(jnp.maximum(jnp.max(mbuf[par], axis=1, keepdims=True), FLOOR) * SCALE, (H, 128))
            mx, st = None, {0: None, 1: None, 'l': None}
            for j in range(2 * (NT + LEAD)):
                if not last and j < 2 * NT:
                    mx = qk_tile(s + 1, 1 - par, j, mx)
                if j >= 2 * LEAD:
                    pv_tile(s, par, j - 2 * LEAD, mk, st)
            if not last:
                mbuf[1 - par] = mx
            a = (st[0] + st[1])[:H]
            l = jnp.broadcast_to(jnp.sum(st['l'], axis=1, keepdims=True), (H, 128))
            put_partial(out, out_i, a[:, :128], a[:, 128:], mk, l)

        for ref in (own_b, recv_1, send_b, recv_2):
            ref[NOWN] = jnp.zeros((2 * H + 8, 128), F32)

        wait(0)
        mx = None
        for j in range(2 * NT):
            mx = qk_tile(0, 0, j, mx)
        mbuf[0] = mx

        def trip(i, last=False):
            s = 2 * i
            wait(s + 1)
            if not last:
                wait(s + 2)

            def when(lag, act):
                if isinstance(i, int):
                    if i >= lag:
                        act()
                else:
                    pl.when(i >= lag)(act)
            when(1, lambda: rcopy_1(i - 1).start())
            when(2, lambda: rcopy_1(i - 2).wait_recv())
            when(3, lambda: rcopy_2(i - 3).start())
            when(6, lambda: rcopy_2(i - 6).wait_recv())
            lagged = lambda lag: jnp.where(i >= lag, i - lag, NOWN)
            half(s, 0, send_a, i)
            combine_1(lagged(2))
            half(s + 1, 1, own_b, i, last=last)
            combine_2(lagged(6))

        def loop_trip(i, _):
            trip(i)
            for u in range(2):
                s = 2 * i + u
                pl.when(s + NB < NREQ)(lambda s=s: start(s + NB))

            @pl.when(i == NREQ // 2 - NB // 2)
            def _():
                for copy in weights[4:]:
                    copy.start()
            return 0
        lax.fori_loop(0, NOWN - 1, loop_trip, 0)
        trip(NOWN - 1, last=True)
        rcopy_1(NOWN - 1).start()
        rcopy_1(NOWN - 2).wait_recv()
        combine_1(NOWN - 2)
        rcopy_2(NOWN - 3).start()
        rcopy_1(NOWN - 1).wait_recv()
        rcopy_2(NOWN - 2).start()
        combine_1(NOWN - 1)
        for i in range(NOWN - 6, NOWN - 3):
            rcopy_2(i).wait_recv()
            if i == NOWN - 6:
                rcopy_2(NOWN - 1).start()
            combine_2(i)
        for i in range(NOWN - 3, NOWN):
            rcopy_2(i).wait_recv()
            combine_2(i)

    attend()

    def output():
        weights[4].wait()
        groups = []
        for g in range(10):
            rhs = jnp.concatenate([wuv[4 * g + k] for k in range(4)], axis=0)
            at = [pl.ds(4 * g + k, NOWN, stride=H) for k in range(4)]
            lhs = jnp.concatenate([jnp.concatenate([ola[r, :], olb[r, :]], axis=1) for r in at], axis=0).astype(BF16)
            v = dot_t(lhs, rhs)
            o = v[3 * NOWN:]
            for k in range(3):
                o = jnp.where(lane256 // 64 == k, v[k * NOWN:(k + 1) * NOWN], o)
            groups.append(o.astype(BF16))
        heads = jnp.concatenate(groups, axis=1)
        weights[5].wait()
        mine = pl.ds(pl.multiple_of(core * NOWN, NOWN), NOWN)

        def xcopy(n):
            piece = xbuf.at[mine, pl.ds(n * 256, 256)]
            return pltpu.make_async_remote_copy(src_ref=piece, dst_ref=piece, send_sem=xs_sem.at[n], recv_sem=xr_sem.at[n],
                                                device_id={'cp': sibling}, device_id_type=pl.DeviceIdType.MESH)

        for n in range(10):
            xbuf[mine, n * 256:(n + 1) * 256] = dot(heads, wo[:, n * 256:(n + 1) * 256])
            if n >= 1:
                xcopy(n - 1).start()
        xcopy(9).start()
        for n in range(10):
            xcopy(n).wait_recv()
        xo_ref[...] = (x_ref[...].astype(F32) + xbuf[...]).astype(BF16)
        for n in range(10):
            xcopy(n).wait_send()

        def sent(i, _):
            rcopy_1(i).wait_send()
            rcopy_2(i).wait_send()
            return 0
        lax.fori_loop(0, NOWN, sent, 0)

    output()


def solution(mesh):
    half_dim = R // 2
    freq = 10000.0 ** (-2.0 * np.arange(half_dim, dtype=np.float64) / R)
    freq = np.tile(freq.astype(np.float32), 8)[None, :]

    def decode_step(x, w_dq, g_q, w_uq, w_dkv, g_kv, w_uk, w_uv, w_o, cache_c, cache_kr, ctx_len):
        vmem, hbm = pl.BlockSpec(memory_space=pltpu.VMEM), pl.BlockSpec(memory_space=pl.ANY)
        dma = pltpu.SemaphoreType.DMA
        part = pltpu.VMEM((NOWN + 1, 2 * H + 8, 128), F32)
        call = pl.pallas_call(
            decode_kernel,
            out_shape=(jax.ShapeDtypeStruct((NREQ, D), BF16), jax.ShapeDtypeStruct((NREQ, L), BF16), jax.ShapeDtypeStruct((NREQ, R), BF16)),
            in_specs=[vmem] * 5 + [pl.BlockSpec(memory_space=pltpu.SMEM)] + [hbm] * 8,
            out_specs=[vmem] * 3,
            scratch_shapes=[
                pltpu.VMEM((D, QL), BF16), pltpu.VMEM((QL, H * 96), BF16), pltpu.VMEM((L + R, D), BF16),
                pltpu.VMEM((H, 64, L), BF16), pltpu.VMEM((H, 64, L), BF16), pltpu.VMEM((H * 64, D), BF16),
                pltpu.VMEM((NB, T, L), BF16), pltpu.VMEM((NB, R, T), BF16),
                pltpu.VMEM((NREQ, H * 96), BF16), pltpu.VMEM((NREQ * H, 128), F32),
                pltpu.VMEM((NREQ, HP, L), BF16), pltpu.VMEM((NREQ, HP, 128), BF16),
                pltpu.VMEM((NREQ, L), F32), pltpu.VMEM((NREQ, 128), F32),
                pltpu.VMEM((2, H, T), F32), pltpu.VMEM((2, H, 128), F32), pltpu.VMEM((NCT, 256, 256), BF16),
                part, part, part, part, part,
                pltpu.VMEM((NREQ * H, 128), F32), pltpu.VMEM((NREQ * H, 128), F32), pltpu.VMEM((NREQ, D), F32),
                dma((6,)), dma((NB,)), dma((NB,)), dma((NOWN,)), dma((NOWN,)), dma((NOWN,)), dma((NOWN,)), dma((10,)), dma((10,)),
            ],
            compiler_params=pltpu.CompilerParams(collective_id=0, has_side_effects=True, vmem_limit_bytes=67_043_328),
        )
        ctx_cols = jnp.broadcast_to(ctx_len[:, None], (NREQ, 128))
        return call(x, g_q[None, :], g_kv[None, :], jnp.asarray(freq), ctx_cols, ctx_len, w_dq, w_uq, w_dkv.T,
                    jnp.transpose(w_uk, (1, 2, 0)), jnp.transpose(w_uv, (1, 2, 0)), w_o, cache_c, jnp.swapaxes(cache_kr, 1, 2))

    rows, cache = P('dp', None), P('dp', 'cp', None)
    in_specs = (rows, P(), P(), P(), P(), P(), P(), P(), P(), cache, cache, P('dp'))
    return jax.shard_map(decode_step, mesh=mesh, in_specs=in_specs, out_specs=(rows, rows, rows), check_vma=False)
```

```python
import functools

import jax
import jax.numpy as jnp
import numpy as np
from jax import lax
from jax.experimental import pallas as pl
from jax.experimental.pallas import tpu as pltpu
from jax.sharding import PartitionSpec as P

F32, BF16 = jnp.float32, jnp.bfloat16
NORM_EPS = 1e-6
SCALE = np.float32(96 ** -0.5 * np.log2(np.e))
MASKED = -2.0e38
FLOOR = -1.0e38

NREQ, T, H, L, R, D, QL = 64, 4096, 40, 256, 32, 2560, 768
HP = 48
NT = 8
NB = 8
NOWN = NREQ // 2
LEAD = 1
NCT = 8
XPOSE_TILES = ((1, 0), (0, 0))


def decode_kernel(x_ref, gq_ref, gkv_ref, freq_ref, ctx_ref, wdq_h, wuq_h, wdkv_h, wuk_h, wuv_h, wo_h, c_h, kr_h,
                  xo_ref, co_ref, ko_ref,
                  wdq, wuq, wdkv, wuk, wuv, wo, cbuf, krbuf, qf, qla, qlb, qrf, qb, qrb, cnf, krf, ctxv,
                  sbuf, mbuf, ctb, send_a, recv_1, own_b, send_b, recv_2, ola, olb, xbuf,
                  wsem, csem, ksem, sa_sem, r1_sem, sb_sem, r2_sem, xs_sem, xr_sem):
    cp = lax.axis_index('cp')
    core = lax.rem(cp, 2)
    sibling = cp + 1 - 2 * core
    mirror = lax.rem(cp + 2, 4)

    barrier = pltpu.get_barrier_semaphore()
    for other in (sibling, mirror):
        pl.semaphore_signal(barrier, inc=1, device_id={'cp': other}, device_id_type=pl.DeviceIdType.MESH)

    weights = [pltpu.make_async_copy(h, v, wsem.at[k]) for k, (h, v) in enumerate(
        ((wdq_h, wdq), (wdkv_h, wdkv), (wuq_h, wuq), (wuk_h, wuk), (wuv_h, wuv), (wo_h, wo)))]

    def request(s):
        u = lax.rem(s, 2)
        half = (1 - core) * (1 - u) + core * u
        return half * NOWN + s // 2

    def cache_copies(s):
        b, slot = request(s), lax.rem(s, NB)
        return (pltpu.make_async_copy(c_h.at[b], cbuf.at[slot], csem.at[slot]),
                pltpu.make_async_copy(kr_h.at[b], krbuf.at[slot], ksem.at[slot]))

    def start(s):
        for copy in cache_copies(s):
            copy.start()

    def wait(s):
        for copy in cache_copies(s):
            copy.wait()

    for copy in weights[:4]:
        copy.start()

    lane128 = lax.broadcasted_iota(jnp.int32, (1, 128), 1)
    lane256 = lax.broadcasted_iota(jnp.int32, (1, 256), 1)

    dot = functools.partial(jnp.dot, preferred_element_type=F32)
    dot_t = functools.partial(lax.dot_general, dimension_numbers=(((1,), (1,)), ((), ())), preferred_element_type=F32)

    def fill(b, _):
        ctxv[pl.ds(b, 1), :] = jnp.full((1, 128), ctx_ref[b], jnp.int32)
        return 0
    lax.fori_loop(0, NREQ, fill, 0)
    angle = ctxv[...].astype(F32) * freq_ref[...]
    cos_t = jnp.cos(angle)
    sin_t = jnp.sin(angle) * jnp.where(lax.rem(lane128, 32) < 16, -1.0, 1.0)

    weights[0].wait()
    cq = [dot(x_ref[...], wdq[:, n * 256:(n + 1) * 256]).astype(BF16).astype(F32) for n in range(3)]
    mean_sq = sum(jnp.sum(v * v, axis=1, keepdims=True) for v in cq) * np.float32(1.0 / QL)
    inv_q = lax.rsqrt(mean_sq + NORM_EPS)
    cn = jnp.concatenate([(cq[n] * inv_q * gq_ref[n * 256:(n + 1) * 256][None, :]).astype(BF16) for n in range(3)], axis=1)

    weights[1].wait()
    kv = dot_t(x_ref[...], wdkv[:L, :])
    inv_kv = lax.rsqrt(jnp.sum(kv * kv, axis=1, keepdims=True) * np.float32(1.0 / L) + NORM_EPS)
    c_new = (kv * inv_kv * gkv_ref[...][None, :]).astype(BF16)
    co_ref[...] = c_new
    cnf[...] = c_new.astype(F32)
    kr = dot_t(x_ref[...], wdkv[L:L + R, :])
    kr = jnp.concatenate([kr, jnp.zeros((NREQ, 128 - R), F32)], axis=1)
    partner = jnp.where(lane128 < 16, pltpu.roll(kr, 112, 1), pltpu.roll(kr, 16, 1))
    kr_new = (kr * cos_t + partner * sin_t).astype(BF16)
    ko_ref[...] = jnp.where(lane128 < R, kr_new, jnp.zeros_like(kr_new))
    krf[...] = jnp.where(lane128 < R, kr_new.astype(F32), 0.0)

    weights[2].wait()
    for s in range(NB):
        start(s)
    for n in range(15):
        qf[:, n * 256:(n + 1) * 256] = dot(cn, wuq[:, n * 256:(n + 1) * 256]).astype(BF16)

    row = lax.broadcasted_iota(jnp.int32, (256, 256), 0)
    col = lax.broadcasted_iota(jnp.int32, (256, 256), 1)
    src = lax.rem(col + jnp.where(col < 128, 0, 16), 32)
    for o in range(8):
        pick = jnp.where(row == src + 32 * o, 1.0, 0.0).astype(BF16)
        heads = [h for h in range(H) if ((96 * h + 64) % 256) // 32 == o]
        wins = [(96 * h + 64) // 256 for h in heads]
        both = dot(jnp.concatenate([qf[:, w * 256:(w + 1) * 256] for w in wins], axis=0), pick)
        for k, h in enumerate(heads):
            part = both[k * NREQ:(k + 1) * NREQ]
            qrf[pl.ds(h, NREQ, stride=H), :] = (part[:, :128] * cos_t + part[:, 128:] * sin_t).astype(BF16).astype(F32)

    weights[3].wait()
    nope = {h: (96 * h, 96 * h + 64) for h in range(H)}
    carry = {}
    for w in range(15):
        lo, hi = 256 * w, 256 * (w + 1)
        here = [(h, max(a, lo), min(b, hi)) for h, (a, b) in nope.items() if a < hi and b > lo]
        pieces, at = [], lo
        for h, a, b in here:
            if a > at:
                pieces.append(jnp.zeros((a - at, 256), BF16))
            pieces.append(wuk[h, a - nope[h][0]:b - nope[h][0], :])
            at = b
        if at < hi:
            pieces.append(jnp.zeros((hi - at, 256), BF16))
        window = qf[:, lo:hi]
        lhs = [window * jnp.where((lane256 >= a - lo) & (lane256 < b - lo), 1.0, 0.0).astype(BF16) for _, a, b in here]
        lat = dot(jnp.concatenate(lhs, axis=0), jnp.concatenate(pieces, axis=0))
        for k, (h, a, b) in enumerate(here):
            v = lat[k * NREQ:(k + 1) * NREQ]
            if a > nope[h][0]:
                v = v + carry.pop(h)
            if b < nope[h][1]:
                carry[h] = v
                continue
            v = v.astype(BF16).astype(F32)
            qla[pl.ds(h, NREQ, stride=H), :] = v[:, :128]
            qlb[pl.ds(h, NREQ, stride=H), :] = v[:, 128:]
    pl.semaphore_wait(barrier, 2)

    def head_rows(i):
        return pl.ds(pl.multiple_of(i * H, 8), H)

    def rcopy_1(i):
        return pltpu.make_async_remote_copy(src_ref=send_a.at[i], dst_ref=recv_1.at[i], send_sem=sa_sem.at[i], recv_sem=r1_sem.at[i],
                                            device_id={'cp': sibling}, device_id_type=pl.DeviceIdType.MESH)

    def rcopy_2(i):
        return pltpu.make_async_remote_copy(src_ref=send_b.at[i], dst_ref=recv_2.at[i], send_sem=sb_sem.at[i], recv_sem=r2_sem.at[i],
                                            device_id={'cp': mirror}, device_id_type=pl.DeviceIdType.MESH)

    def put_partial(ref, i, lo, hi, m, l):
        ref[i, 0:H, :] = lo
        ref[i, H:2 * H, :] = hi
        ml = jnp.zeros((8, 128), F32)
        for g in range(5):
            ml = jnp.where(lane128 == g, m[8 * g:8 * g + 8], ml)
            ml = jnp.where(lane128 == 8 + g, l[8 * g:8 * g + 8], ml)
        ref[i, 2 * H:2 * H + 8, :] = ml

    def get_partial(ref, i):
        ml = ref[i, 2 * H:2 * H + 8, :]
        spread = lambda at: jnp.concatenate([jnp.broadcast_to(ml[:, at + g:at + g + 1], (8, 128)) for g in range(5)], axis=0)
        return ref[i, 0:H, :], ref[i, H:2 * H, :], spread(0), spread(8)

    def combine_1(i):
        lo_p, hi_p, m_p, l_p = get_partial(own_b, i)
        lo_q, hi_q, m_q, l_q = get_partial(recv_1, i)
        m = jnp.maximum(m_p, m_q)
        f_p, f_q = jnp.exp2(m_p - m), jnp.exp2(m_q - m)
        put_partial(send_b, i, lo_p * f_p + lo_q * f_q, hi_p * f_p + hi_q * f_q, m, l_p * f_p + l_q * f_q)

    def combine_2(i):
        lo_p, hi_p, m_p, l_p = get_partial(send_b, i)
        lo_q, hi_q, m_q, l_q = get_partial(recv_2, i)
        ii = jnp.minimum(i, NOWN - 1)
        b = core * NOWN + ii
        c_row, k_row = cnf[pl.ds(b, 1), :], krf[pl.ds(b, 1), :]
        mine = head_rows(b)
        part = qla[mine, :] * c_row[:, :128] + qlb[mine, :] * c_row[:, 128:] + qrf[mine, :] * k_row
        s_new = jnp.broadcast_to(jnp.sum(part, axis=1, keepdims=True) * SCALE, (H, 128))
        m = jnp.maximum(jnp.maximum(m_p, m_q), s_new)
        f_p, f_q, w_new = jnp.exp2(m_p - m), jnp.exp2(m_q - m), jnp.exp2(s_new - m)
        inv = 1.0 / (l_p * f_p + l_q * f_q + w_new)
        w_new = w_new.astype(BF16).astype(F32)
        rows = head_rows(i)
        ola[rows, :] = (lo_p * f_p + lo_q * f_q + w_new * c_row[:, :128]) * inv
        olb[rows, :] = (hi_p * f_p + hi_q * f_q + w_new * c_row[:, 128:]) * inv

    def attend():
        count = [0]

        def load_q(s, par):
            rows = head_rows(request(s))
            q = jnp.concatenate([qla[rows, :], qlb[rows, :]], axis=1)
            qb[par] = jnp.concatenate([q, jnp.zeros((HP - H, L), F32)], axis=0).astype(BF16)
            qrb[par] = jnp.concatenate([qrf[rows, :], jnp.zeros((HP - H, 128), F32)], axis=0).astype(BF16)

        def qk_tile(s, par, j, mx):
            slot, b = lax.rem(s, NB), request(s)
            n = ctx_ref[b] - cp * T
            at = pl.ds(256 * j, 256)
            c = cbuf[slot, at, :]
            if (par, j // 2) in XPOSE_TILES:
                v = dot_t(qb[par], c)
            else:
                t = count[0] % NCT
                count[0] += 1
                ctb[t] = c.T
                v = dot(qb[par], ctb[t])
            v = (v + dot(qrb[par, :, :R], krbuf[slot, :, at]))[:H]
            v = jnp.where(lane256 + j * 256 < n, v, MASKED)
            sbuf[par, :, at] = v
            for k in range(2):
                part = v[:, k * 128:(k + 1) * 128]
                mx = part if mx is None else jnp.maximum(mx, part)
            return mx

        def pv_tile(s, par, j, mk, st):
            ws = []
            for k in range(2):
                w = jnp.exp2(sbuf[par, :, pl.ds(j * 256 + k * 128, 128)] * SCALE - mk)
                st['l'] = w if st['l'] is None else st['l'] + w
                ws.append(w)
            w = jnp.concatenate([jnp.concatenate(ws, axis=1), jnp.zeros((HP - H, 256), F32)], axis=0).astype(BF16)
            p = dot(w, cbuf[lax.rem(s, NB), pl.ds(256 * j, 256), :])
            st[j % 2] = p if st[j % 2] is None else st[j % 2] + p

        def half(s, par, out, out_i, last=False):
            mk = jnp.broadcast_to(jnp.maximum(jnp.max(mbuf[par], axis=1, keepdims=True), FLOOR) * SCALE, (H, 128))
            mx, st = None, {0: None, 1: None, 'l': None}
            if not last:
                load_q(s + 1, 1 - par)
            for j in range(2 * (NT + LEAD)):
                if not last and j < 2 * NT:
                    mx = qk_tile(s + 1, 1 - par, j, mx)
                if j >= 2 * LEAD:
                    pv_tile(s, par, j - 2 * LEAD, mk, st)
            if not last:
                mbuf[1 - par] = mx
            a = (st[0] + st[1])[:H]
            l = jnp.broadcast_to(jnp.sum(st['l'], axis=1, keepdims=True), (H, 128))
            put_partial(out, out_i, a[:, :128], a[:, 128:], mk, l)

        for ref in (own_b, recv_1, send_b, recv_2):
            ref[NOWN] = jnp.zeros((2 * H + 8, 128), F32)

        wait(0)
        load_q(0, 0)
        mx = None
        for j in range(2 * NT):
            mx = qk_tile(0, 0, j, mx)
        mbuf[0] = mx

        def trip(i, last=False):
            s = 2 * i
            wait(s + 1)
            if not last:
                wait(s + 2)

            def when(lag, act):
                if isinstance(i, int):
                    if i >= lag:
                        act()
                else:
                    pl.when(i >= lag)(act)
            when(1, lambda: rcopy_1(i - 1).start())
            when(2, lambda: rcopy_1(i - 2).wait_recv())
            when(3, lambda: rcopy_2(i - 3).start())
            when(6, lambda: rcopy_2(i - 6).wait_recv())
            lagged = lambda lag: jnp.where(i >= lag, i - lag, NOWN)
            half(s, 0, send_a, i)
            combine_1(lagged(2))
            half(s + 1, 1, own_b, i, last=last)
            combine_2(lagged(6))

        def loop_trip(i, _):
            trip(i)
            for u in range(2):
                s = 2 * i + u
                pl.when(s + NB < NREQ)(lambda s=s: start(s + NB))

            @pl.when(i == NREQ // 2 - NB // 2)
            def _():
                for copy in weights[4:]:
                    copy.start()
            return 0
        lax.fori_loop(0, NOWN - 1, loop_trip, 0)
        trip(NOWN - 1, last=True)
        rcopy_1(NOWN - 1).start()
        rcopy_1(NOWN - 2).wait_recv()
        combine_1(NOWN - 2)
        rcopy_2(NOWN - 3).start()
        rcopy_1(NOWN - 1).wait_recv()
        rcopy_2(NOWN - 2).start()
        combine_1(NOWN - 1)
        for i in range(NOWN - 6, NOWN - 3):
            rcopy_2(i).wait_recv()
            if i == NOWN - 6:
                rcopy_2(NOWN - 1).start()
            combine_2(i)
        for i in range(NOWN - 3, NOWN):
            rcopy_2(i).wait_recv()
            combine_2(i)

    attend()

    def output():
        weights[4].wait()
        groups = []
        for g in range(10):
            rhs = jnp.concatenate([wuv[4 * g + k] for k in range(4)], axis=0)
            at = [pl.ds(4 * g + k, NOWN, stride=H) for k in range(4)]
            lhs = jnp.concatenate([jnp.concatenate([ola[r, :], olb[r, :]], axis=1) for r in at], axis=0).astype(BF16)
            v = dot_t(lhs, rhs)
            o = v[3 * NOWN:]
            for k in range(3):
                o = jnp.where(lane256 // 64 == k, v[k * NOWN:(k + 1) * NOWN], o)
            groups.append(o.astype(BF16))
        heads = jnp.concatenate(groups, axis=1)
        weights[5].wait()
        mine = pl.ds(pl.multiple_of(core * NOWN, NOWN), NOWN)

        def xcopy(n):
            piece = xbuf.at[mine, pl.ds(n * 256, 256)]
            return pltpu.make_async_remote_copy(src_ref=piece, dst_ref=piece, send_sem=xs_sem.at[n], recv_sem=xr_sem.at[n],
                                                device_id={'cp': sibling}, device_id_type=pl.DeviceIdType.MESH)

        for n in range(10):
            xbuf[mine, n * 256:(n + 1) * 256] = dot(heads, wo[:, n * 256:(n + 1) * 256])
            if n >= 1:
                xcopy(n - 1).start()
        xcopy(9).start()
        for n in range(10):
            xcopy(n).wait_recv()
        xo_ref[...] = (x_ref[...].astype(F32) + xbuf[...]).astype(BF16)
        for n in range(10):
            xcopy(n).wait_send()

        def sent(i, _):
            rcopy_1(i).wait_send()
            rcopy_2(i).wait_send()
            return 0
        lax.fori_loop(0, NOWN, sent, 0)

    output()


def finish_kernel(x_ref, c_ref, k_ref, xo_ref, co_ref, ko_ref):
    xo_ref[...] = x_ref[...]
    co_ref[...] = c_ref[...]
    ko_ref[...] = k_ref[...].astype(F32).T[:R].astype(BF16)


def solution(mesh):
    half_dim = R // 2
    freq = 10000.0 ** (-2.0 * np.arange(half_dim, dtype=np.float64) / R)
    freq = np.tile(freq.astype(np.float32), 8)[None, :]

    def decode_step(x, w_dq, g_q, w_uq, w_dkv, g_kv, w_uk, w_uv, w_o, cache_c, cache_kr, ctx_len):
        vmem, hbm = pl.BlockSpec(memory_space=pltpu.VMEM), pl.BlockSpec(memory_space=pl.ANY)
        dma = pltpu.SemaphoreType.DMA
        part = pltpu.VMEM((NOWN + 1, 2 * H + 8, 128), F32)
        call = pl.pallas_call(
            decode_kernel,
            out_shape=(jax.ShapeDtypeStruct((NREQ, D), BF16), jax.ShapeDtypeStruct((NREQ, L), BF16), jax.ShapeDtypeStruct((NREQ, 128), BF16)),
            in_specs=[vmem] * 4 + [pl.BlockSpec(memory_space=pltpu.SMEM)] + [hbm] * 8,
            out_specs=[vmem] * 3,
            scratch_shapes=[
                pltpu.VMEM((D, QL), BF16), pltpu.VMEM((QL, H * 96), BF16), pltpu.VMEM((L + R, D), BF16),
                pltpu.VMEM((H, 64, L), BF16), pltpu.VMEM((H, 64, L), BF16), pltpu.VMEM((H * 64, D), BF16),
                pltpu.VMEM((NB, T, L), BF16), pltpu.VMEM((NB, R, T), BF16),
                pltpu.VMEM((NREQ, H * 96), BF16), pltpu.VMEM((NREQ * H, 128), F32), pltpu.VMEM((NREQ * H, 128), F32), pltpu.VMEM((NREQ * H, 128), F32),
                pltpu.VMEM((2, HP, L), BF16), pltpu.VMEM((2, HP, 128), BF16),
                pltpu.VMEM((NREQ, L), F32), pltpu.VMEM((NREQ, 128), F32), pltpu.VMEM((NREQ, 128), jnp.int32),
                pltpu.VMEM((2, H, T), F32), pltpu.VMEM((2, H, 128), F32), pltpu.VMEM((NCT, 256, 256), BF16),
                part, part, part, part, part,
                pltpu.VMEM(((NOWN + 1) * H, 128), F32), pltpu.VMEM(((NOWN + 1) * H, 128), F32), pltpu.VMEM((NREQ, D), F32),
                dma((6,)), dma((NB,)), dma((NB,)), dma((NOWN,)), dma((NOWN,)), dma((NOWN,)), dma((NOWN,)), dma((10,)), dma((10,)),
            ],
            compiler_params=pltpu.CompilerParams(collective_id=0, has_side_effects=True, vmem_limit_bytes=67_043_328),
        )
        outs = call(x, g_q, g_kv, jnp.asarray(freq), ctx_len, w_dq, w_uq, w_dkv.T,
                    jnp.transpose(w_uk, (1, 2, 0)), jnp.transpose(w_uv, (1, 2, 0)), w_o, cache_c, jnp.swapaxes(cache_kr, 1, 2))
        shapes = [jax.ShapeDtypeStruct(shape, BF16) for shape in ((NREQ, D), (NREQ, L), (R, NREQ))]
        x_out, c_new, kr_new = pl.pallas_call(finish_kernel, out_shape=shapes, in_specs=[vmem] * 3, out_specs=[vmem] * 3)(*outs)
        return x_out, c_new, kr_new.T

    rows, cache = P('dp', None), P('dp', 'cp', None)
    in_specs = (rows, P(), P(), P(), P(), P(), P(), P(), P(), cache, cache, P('dp'))
    return jax.shard_map(decode_step, mesh=mesh, in_specs=in_specs, out_specs=(rows, rows, rows), check_vma=False)
```

```python
import functools

import jax
import jax.numpy as jnp
import numpy as np
from jax import lax
from jax.experimental import pallas as pl
from jax.experimental.pallas import tpu as pltpu
from jax.sharding import PartitionSpec as P

F32, BF16 = jnp.float32, jnp.bfloat16
NORM_EPS = 1e-6
SCALE = np.float32(96 ** -0.5 * np.log2(np.e))
MASKED = -2.0e38
FLOOR = -1.0e38

NREQ, T, H, L, R, D, QL = 64, 4096, 40, 256, 32, 2560, 768
HP = 48
NT = 8
NB = 8
NOWN = NREQ // 2
LEAD = 1
NCT = 8
XPOSE_TILES = ((1, 0), (0, 0))


def decode_kernel(x_ref, gq_ref, gkv_ref, freq_ref, ctx_ref, wdq_h, wuq_h, wdkv_h, wuk_h, wuv_h, wo_h, c_h, kr_h,
                  xo_ref, co_ref, ko_ref,
                  wdq, wuq, wdkv, wuk, wuv, wo, cbuf, krbuf, qf, qla, qlb, qrf, qb, qrb, cnf, krf, ctxv,
                  sbuf, mbuf, ctb, send_a, recv_1, own_b, send_b, recv_2, ola, olb, xbuf,
                  wsem, csem, ksem, sa_sem, r1_sem, sb_sem, r2_sem, xs_sem, xr_sem):
    cp = lax.axis_index('cp')
    core = lax.rem(cp, 2)
    sibling = cp + 1 - 2 * core
    mirror = lax.rem(cp + 2, 4)

    barrier = pltpu.get_barrier_semaphore()
    for other in (sibling, mirror):
        pl.semaphore_signal(barrier, inc=1, device_id={'cp': other}, device_id_type=pl.DeviceIdType.MESH)

    weights = [pltpu.make_async_copy(h, v, wsem.at[k]) for k, (h, v) in enumerate(
        ((wdq_h, wdq), (wdkv_h, wdkv), (wuq_h, wuq), (wuk_h, wuk), (wuv_h, wuv), (wo_h, wo)))]

    def request(s):
        u = lax.rem(s, 2)
        half = (1 - core) * (1 - u) + core * u
        return half * NOWN + s // 2

    def cache_copies(s):
        b, slot = request(s), lax.rem(s, NB)
        return (pltpu.make_async_copy(c_h.at[b], cbuf.at[slot], csem.at[slot]),
                pltpu.make_async_copy(kr_h.at[b], krbuf.at[slot], ksem.at[slot]))

    def start(s):
        for copy in cache_copies(s):
            copy.start()

    def wait(s):
        for copy in cache_copies(s):
            copy.wait()

    for copy in weights[:4]:
        copy.start()

    lane128 = lax.broadcasted_iota(jnp.int32, (1, 128), 1)
    lane256 = lax.broadcasted_iota(jnp.int32, (1, 256), 1)

    dot = functools.partial(jnp.dot, preferred_element_type=F32)
    dot_t = functools.partial(lax.dot_general, dimension_numbers=(((1,), (1,)), ((), ())), preferred_element_type=F32)

    def fill(b, _):
        ctxv[pl.ds(b, 1), :] = jnp.full((1, 128), ctx_ref[b], jnp.int32)
        return 0
    lax.fori_loop(0, NREQ, fill, 0)
    angle = ctxv[...].astype(F32) * freq_ref[...]
    cos_t = jnp.cos(angle)
    sin_t = jnp.sin(angle) * jnp.where(lax.rem(lane128, 32) < 16, -1.0, 1.0)

    weights[0].wait()
    cq = [dot(x_ref[...], wdq[:, n * 256:(n + 1) * 256]).astype(BF16).astype(F32) for n in range(3)]
    mean_sq = sum(jnp.sum(v * v, axis=1, keepdims=True) for v in cq) * np.float32(1.0 / QL)
    inv_q = lax.rsqrt(mean_sq + NORM_EPS)
    cn = jnp.concatenate([(cq[n] * inv_q * gq_ref[n * 256:(n + 1) * 256][None, :]).astype(BF16) for n in range(3)], axis=1)

    weights[1].wait()
    kv = dot_t(x_ref[...], wdkv[:L, :])
    inv_kv = lax.rsqrt(jnp.sum(kv * kv, axis=1, keepdims=True) * np.float32(1.0 / L) + NORM_EPS)
    c_new = (kv * inv_kv * gkv_ref[...][None, :]).astype(BF16)
    co_ref[...] = c_new
    cnf[...] = c_new.astype(F32)
    kr = dot_t(x_ref[...], wdkv[L:L + R, :])
    kr = jnp.concatenate([kr, jnp.zeros((NREQ, 128 - R), F32)], axis=1)
    partner = jnp.where(lane128 < 16, pltpu.roll(kr, 112, 1), pltpu.roll(kr, 16, 1))
    kr_new = (kr * cos_t + partner * sin_t).astype(BF16)
    ko_ref[...] = jnp.where(lane128 < R, kr_new, jnp.zeros_like(kr_new))
    krf[...] = jnp.where(lane128 < R, kr_new.astype(F32), 0.0)

    weights[2].wait()
    for s in range(NB):
        start(s)
    for n in range(15):
        qf[:, n * 256:(n + 1) * 256] = dot(cn, wuq[:, n * 256:(n + 1) * 256]).astype(BF16)

    row = lax.broadcasted_iota(jnp.int32, (256, 256), 0)
    col = lax.broadcasted_iota(jnp.int32, (256, 256), 1)
    src = lax.rem(col + jnp.where(col < 128, 0, 16), 32)
    for o in range(8):
        pick = jnp.where(row == src + 32 * o, 1.0, 0.0).astype(BF16)
        heads = [h for h in range(H) if ((96 * h + 64) % 256) // 32 == o]
        wins = [(96 * h + 64) // 256 for h in heads]
        both = dot(jnp.concatenate([qf[:, w * 256:(w + 1) * 256] for w in wins], axis=0), pick)
        for k, h in enumerate(heads):
            part = both[k * NREQ:(k + 1) * NREQ]
            qrf[pl.ds(h, NREQ, stride=H), :] = (part[:, :128] * cos_t + part[:, 128:] * sin_t).astype(BF16).astype(F32)

    weights[3].wait()
    nope = {h: (96 * h, 96 * h + 64) for h in range(H)}
    carry = {}
    for w in range(15):
        lo, hi = 256 * w, 256 * (w + 1)
        here = [(h, max(a, lo), min(b, hi)) for h, (a, b) in nope.items() if a < hi and b > lo]
        pieces, at = [], lo
        for h, a, b in here:
            if a > at:
                pieces.append(jnp.zeros((a - at, 256), BF16))
            pieces.append(wuk[h, a - nope[h][0]:b - nope[h][0], :])
            at = b
        if at < hi:
            pieces.append(jnp.zeros((hi - at, 256), BF16))
        window = qf[:, lo:hi]
        lhs = [window * jnp.where((lane256 >= a - lo) & (lane256 < b - lo), 1.0, 0.0).astype(BF16) for _, a, b in here]
        lat = dot(jnp.concatenate(lhs, axis=0), jnp.concatenate(pieces, axis=0))
        for k, (h, a, b) in enumerate(here):
            v = lat[k * NREQ:(k + 1) * NREQ]
            if a > nope[h][0]:
                v = v + carry.pop(h)
            if b < nope[h][1]:
                carry[h] = v
                continue
            v = v.astype(BF16).astype(F32)
            qla[pl.ds(h, NREQ, stride=H), :] = v[:, :128]
            qlb[pl.ds(h, NREQ, stride=H), :] = v[:, 128:]
    pl.semaphore_wait(barrier, 2)

    def head_rows(i):
        return pl.ds(pl.multiple_of(i * H, 8), H)

    def rcopy_1(i):
        return pltpu.make_async_remote_copy(src_ref=send_a.at[i], dst_ref=recv_1.at[i], send_sem=sa_sem.at[i], recv_sem=r1_sem.at[i],
                                            device_id={'cp': sibling}, device_id_type=pl.DeviceIdType.MESH)

    def rcopy_2(i):
        return pltpu.make_async_remote_copy(src_ref=send_b.at[i], dst_ref=recv_2.at[i], send_sem=sb_sem.at[i], recv_sem=r2_sem.at[i],
                                            device_id={'cp': mirror}, device_id_type=pl.DeviceIdType.MESH)

    def put_partial(ref, i, lo, hi, m, l):
        ref[i, 0:H, :] = lo
        ref[i, H:2 * H, :] = hi
        ml = jnp.zeros((8, 128), F32)
        for g in range(5):
            ml = jnp.where(lane128 == g, m[8 * g:8 * g + 8], ml)
            ml = jnp.where(lane128 == 8 + g, l[8 * g:8 * g + 8], ml)
        ref[i, 2 * H:2 * H + 8, :] = ml

    def get_partial(ref, i):
        ml = ref[i, 2 * H:2 * H + 8, :]
        spread = lambda at: jnp.concatenate([jnp.broadcast_to(ml[:, at + g:at + g + 1], (8, 128)) for g in range(5)], axis=0)
        return ref[i, 0:H, :], ref[i, H:2 * H, :], spread(0), spread(8)

    def combine_1(i):
        lo_p, hi_p, m_p, l_p = get_partial(own_b, i)
        lo_q, hi_q, m_q, l_q = get_partial(recv_1, i)
        m = jnp.maximum(m_p, m_q)
        f_p, f_q = jnp.exp2(m_p - m), jnp.exp2(m_q - m)
        put_partial(send_b, i, lo_p * f_p + lo_q * f_q, hi_p * f_p + hi_q * f_q, m, l_p * f_p + l_q * f_q)

    def combine_2(i):
        lo_p, hi_p, m_p, l_p = get_partial(send_b, i)
        lo_q, hi_q, m_q, l_q = get_partial(recv_2, i)
        ii = jnp.minimum(i, NOWN - 1)
        b = core * NOWN + ii
        c_row, k_row = cnf[pl.ds(b, 1), :], krf[pl.ds(b, 1), :]
        mine = head_rows(b)
        part = qla[mine, :] * c_row[:, :128] + qlb[mine, :] * c_row[:, 128:] + qrf[mine, :] * k_row
        s_new = jnp.broadcast_to(jnp.sum(part, axis=1, keepdims=True) * SCALE, (H, 128))
        m = jnp.maximum(jnp.maximum(m_p, m_q), s_new)
        f_p, f_q, w_new = jnp.exp2(m_p - m), jnp.exp2(m_q - m), jnp.exp2(s_new - m)
        inv = 1.0 / (l_p * f_p + l_q * f_q + w_new)
        w_new = w_new.astype(BF16).astype(F32)
        rows = head_rows(i)
        ola[rows, :] = (lo_p * f_p + lo_q * f_q + w_new * c_row[:, :128]) * inv
        olb[rows, :] = (hi_p * f_p + hi_q * f_q + w_new * c_row[:, 128:]) * inv

    def attend():
        count = [0]

        def load_q(s, par):
            rows = head_rows(request(s))
            q = jnp.concatenate([qla[rows, :], qlb[rows, :]], axis=1)
            qb[par] = jnp.concatenate([q, jnp.zeros((HP - H, L), F32)], axis=0).astype(BF16)
            qrb[par] = jnp.concatenate([qrf[rows, :], jnp.zeros((HP - H, 128), F32)], axis=0).astype(BF16)

        def qk_tile(s, par, j, mx):
            slot, b = lax.rem(s, NB), request(s)
            n = ctx_ref[b] - cp * T
            at = pl.ds(256 * j, 256)
            c = cbuf[slot, at, :]
            if (par, j // 2) in XPOSE_TILES:
                v = dot_t(qb[par], c)
            else:
                t = count[0] % NCT
                count[0] += 1
                ctb[t] = c.T
                v = dot(qb[par], ctb[t])
            v = (v + dot(qrb[par, :, :R], krbuf[slot, :, at]))[:H]
            v = jnp.where(lane256 + j * 256 < n, v, MASKED)
            sbuf[par, :, at] = v
            for k in range(2):
                part = v[:, k * 128:(k + 1) * 128]
                mx = part if mx is None else jnp.maximum(mx, part)
            return mx

        def pv_tile(s, par, j, mk, st):
            ws = []
            for k in range(2):
                w = jnp.exp2(sbuf[par, :, pl.ds(j * 256 + k * 128, 128)] * SCALE - mk)
                st['l'] = w if st['l'] is None else st['l'] + w
                ws.append(w)
            w = jnp.concatenate([jnp.concatenate(ws, axis=1), jnp.zeros((HP - H, 256), F32)], axis=0).astype(BF16)
            p = dot(w, cbuf[lax.rem(s, NB), pl.ds(256 * j, 256), :])
            st[j % 2] = p if st[j % 2] is None else st[j % 2] + p

        def half(s, par, out, out_i, last=False):
            mk = jnp.broadcast_to(jnp.maximum(jnp.max(mbuf[par], axis=1, keepdims=True), FLOOR) * SCALE, (H, 128))
            mx, st = None, {0: None, 1: None, 'l': None}
            if not last:
                load_q(s + 1, 1 - par)
            for j in range(2 * (NT + LEAD)):
                if not last and j < 2 * NT:
                    mx = qk_tile(s + 1, 1 - par, j, mx)
                if j >= 2 * LEAD:
                    pv_tile(s, par, j - 2 * LEAD, mk, st)
            if not last:
                mbuf[1 - par] = mx
            a = (st[0] + st[1])[:H]
            l = jnp.broadcast_to(jnp.sum(st['l'], axis=1, keepdims=True), (H, 128))
            put_partial(out, out_i, a[:, :128], a[:, 128:], mk, l)

        for ref in (own_b, recv_1, send_b, recv_2):
            ref[NOWN] = jnp.zeros((2 * H + 8, 128), F32)

        wait(0)
        load_q(0, 0)
        mx = None
        for j in range(2 * NT):
            mx = qk_tile(0, 0, j, mx)
        mbuf[0] = mx

        def trip(i, last=False):
            s = 2 * i
            wait(s + 1)
            if not last:
                wait(s + 2)

            def when(lag, act):
                if isinstance(i, int):
                    if i >= lag:
                        act()
                else:
                    pl.when(i >= lag)(act)
            when(1, lambda: rcopy_1(i - 1).start())
            when(2, lambda: rcopy_1(i - 2).wait_recv())
            when(3, lambda: rcopy_2(i - 3).start())
            when(6, lambda: rcopy_2(i - 6).wait_recv())
            lagged = lambda lag: jnp.where(i >= lag, i - lag, NOWN)
            half(s, 0, send_a, i)
            combine_1(lagged(2))
            if last:
                rcopy_1(i).start()
                rcopy_1(i - 1).wait_recv()
                combine_1(i - 1)
                rcopy_2(i - 2).start()
            half(s + 1, 1, own_b, i, last=last)
            combine_2(lagged(6))

        def loop_trip(i, _):
            trip(i)
            for u in range(2):
                s = 2 * i + u
                pl.when(s + NB < NREQ)(lambda s=s: start(s + NB))

            @pl.when(i == NREQ // 2 - NB // 2)
            def _():
                for copy in weights[4:]:
                    copy.start()
            return 0
        lax.fori_loop(0, NOWN - 1, loop_trip, 0)
        trip(NOWN - 1, last=True)
        rcopy_1(NOWN - 1).wait_recv()
        rcopy_2(NOWN - 2).start()
        combine_1(NOWN - 1)
        for i in range(NOWN - 6, NOWN):
            rcopy_2(i).wait_recv()
            combine_2(i)
            if i == NOWN - 6:
                rcopy_2(NOWN - 1).start()

    attend()

    def output():
        weights[4].wait()
        groups = []
        for g in range(10):
            rhs = jnp.concatenate([wuv[4 * g + k] for k in range(4)], axis=0)
            at = [pl.ds(4 * g + k, NOWN, stride=H) for k in range(4)]
            lhs = jnp.concatenate([jnp.concatenate([ola[r, :], olb[r, :]], axis=1) for r in at], axis=0).astype(BF16)
            v = dot_t(lhs, rhs)
            o = v[3 * NOWN:]
            for k in range(3):
                o = jnp.where(lane256 // 64 == k, v[k * NOWN:(k + 1) * NOWN], o)
            groups.append(o.astype(BF16))
        heads = jnp.concatenate(groups, axis=1)
        weights[5].wait()
        mine = pl.ds(pl.multiple_of(core * NOWN, NOWN), NOWN)

        def xcopy(n):
            piece = xbuf.at[mine, pl.ds(n * 1280, 1280)]
            return pltpu.make_async_remote_copy(src_ref=piece, dst_ref=piece, send_sem=xs_sem.at[n], recv_sem=xr_sem.at[n],
                                                device_id={'cp': sibling}, device_id_type=pl.DeviceIdType.MESH)

        for n in range(2):
            for k in range(5 * n, 5 * n + 5):
                xbuf[mine, k * 256:(k + 1) * 256] = dot(heads, wo[:, k * 256:(k + 1) * 256])
            xcopy(n).start()
        for n in range(2):
            xcopy(n).wait_recv()
        xo_ref[...] = (x_ref[...].astype(F32) + xbuf[...]).astype(BF16)
        for n in range(2):
            xcopy(n).wait_send()

        def sent(i, _):
            rcopy_1(i).wait_send()
            rcopy_2(i).wait_send()
            return 0
        lax.fori_loop(0, NOWN, sent, 0)

    output()


def finish_kernel(x_ref, c_ref, k_ref, xo_ref, co_ref, ko_ref):
    xo_ref[...] = x_ref[...]
    co_ref[...] = c_ref[...]
    ko_ref[...] = k_ref[...].astype(F32).T[:R].astype(BF16)


def solution(mesh):
    half_dim = R // 2
    freq = 10000.0 ** (-2.0 * np.arange(half_dim, dtype=np.float64) / R)
    freq = np.tile(freq.astype(np.float32), 8)[None, :]

    def decode_step(x, w_dq, g_q, w_uq, w_dkv, g_kv, w_uk, w_uv, w_o, cache_c, cache_kr, ctx_len):
        vmem, hbm = pl.BlockSpec(memory_space=pltpu.VMEM), pl.BlockSpec(memory_space=pl.ANY)
        dma = pltpu.SemaphoreType.DMA
        part = pltpu.VMEM((NOWN + 1, 2 * H + 8, 128), F32)
        call = pl.pallas_call(
            decode_kernel,
            out_shape=(jax.ShapeDtypeStruct((NREQ, D), BF16), jax.ShapeDtypeStruct((NREQ, L), BF16), jax.ShapeDtypeStruct((NREQ, 128), BF16)),
            in_specs=[vmem] * 4 + [pl.BlockSpec(memory_space=pltpu.SMEM)] + [hbm] * 8,
            out_specs=[vmem] * 3,
            scratch_shapes=[
                pltpu.VMEM((D, QL), BF16), pltpu.VMEM((QL, H * 96), BF16), pltpu.VMEM((L + R, D), BF16),
                pltpu.VMEM((H, 64, L), BF16), pltpu.VMEM((H, 64, L), BF16), pltpu.VMEM((H * 64, D), BF16),
                pltpu.VMEM((NB, T, L), BF16), pltpu.VMEM((NB, R, T), BF16),
                pltpu.VMEM((NREQ, H * 96), BF16), pltpu.VMEM((NREQ * H, 128), F32), pltpu.VMEM((NREQ * H, 128), F32), pltpu.VMEM((NREQ * H, 128), F32),
                pltpu.VMEM((2, HP, L), BF16), pltpu.VMEM((2, HP, 128), BF16),
                pltpu.VMEM((NREQ, L), F32), pltpu.VMEM((NREQ, 128), F32), pltpu.VMEM((NREQ, 128), jnp.int32),
                pltpu.VMEM((2, H, T), F32), pltpu.VMEM((2, H, 128), F32), pltpu.VMEM((NCT, 256, 256), BF16),
                part, part, part, part, part,
                pltpu.VMEM(((NOWN + 1) * H, 128), F32), pltpu.VMEM(((NOWN + 1) * H, 128), F32), pltpu.VMEM((NREQ, D), F32),
                dma((6,)), dma((NB,)), dma((NB,)), dma((NOWN,)), dma((NOWN,)), dma((NOWN,)), dma((NOWN,)), dma((10,)), dma((10,)),
            ],
            compiler_params=pltpu.CompilerParams(collective_id=0, has_side_effects=True, vmem_limit_bytes=67_043_328),
        )
        outs = call(x, g_q, g_kv, jnp.asarray(freq), ctx_len, w_dq, w_uq, w_dkv.T,
                    jnp.transpose(w_uk, (1, 2, 0)), jnp.transpose(w_uv, (1, 2, 0)), w_o, cache_c, jnp.swapaxes(cache_kr, 1, 2))
        shapes = [jax.ShapeDtypeStruct(shape, BF16) for shape in ((NREQ, D), (NREQ, L), (R, NREQ))]
        x_out, c_new, kr_new = pl.pallas_call(finish_kernel, out_shape=shapes, in_specs=[vmem] * 3, out_specs=[vmem] * 3)(*outs)
        return x_out, c_new, kr_new.T

    rows, cache = P('dp', None), P('dp', 'cp', None)
    in_specs = (rows, P(), P(), P(), P(), P(), P(), P(), P(), cache, cache, P('dp'))
    return jax.shard_map(decode_step, mesh=mesh, in_specs=in_specs, out_specs=(rows, rows, rows), check_vma=False)
```

```python
import functools

import jax
import jax.numpy as jnp
import numpy as np
from jax import lax
from jax.experimental import pallas as pl
from jax.experimental.pallas import tpu as pltpu
from jax.sharding import PartitionSpec as P

F32, BF16 = jnp.float32, jnp.bfloat16
NORM_EPS = 1e-6
SCALE = np.float32(96 ** -0.5 * np.log2(np.e))
MASKED = -2.0e38
FLOOR = -1.0e38

NREQ, T, H, L, R, D, QL = 64, 4096, 40, 256, 32, 2560, 768
HP = 48
NT = 8
NB = 8
NOWN = NREQ // 2
LEAD = 4
XPOSE_TILES = ((1, 0), (0, 0))


def decode_kernel(x_ref, gq_ref, gkv_ref, freq_ref, ctx_ref, wdq_h, wuq_h, wdkv_h, wuk_h, wuv_h, wo_h, c_h, kr_h,
                  xo_ref, co_ref, ko_ref,
                  wdq, wuq, wdkv, wuk, wuv, wo, cbuf, krbuf, qf, qla, qlb, qrf, qb, qrb, cnf, krf, ctxv,
                  sbuf, mbuf, send_a, recv_1, own_b, send_b, recv_2, ola, olb, xbuf,
                  wsem, csem, ksem, sa_sem, r1_sem, sb_sem, r2_sem, xs_sem, xr_sem):
    cp = lax.axis_index('cp')
    core = lax.rem(cp, 2)
    sibling = cp + 1 - 2 * core
    mirror = lax.rem(cp + 2, 4)

    barrier = pltpu.get_barrier_semaphore()
    for other in (sibling, mirror):
        pl.semaphore_signal(barrier, inc=1, device_id={'cp': other}, device_id_type=pl.DeviceIdType.MESH)

    weights = [pltpu.make_async_copy(h, v, wsem.at[k]) for k, (h, v) in enumerate(
        ((wdq_h, wdq), (wdkv_h, wdkv), (wuq_h, wuq), (wuk_h, wuk), (wuv_h, wuv), (wo_h, wo)))]

    def request(s):
        u = lax.rem(s, 2)
        half = (1 - core) * (1 - u) + core * u
        return half * NOWN + s // 2

    def cache_copies(s):
        b, slot = request(s), lax.rem(s, NB)
        return (pltpu.make_async_copy(c_h.at[b], cbuf.at[slot], csem.at[slot]),
                pltpu.make_async_copy(kr_h.at[b], krbuf.at[slot], ksem.at[slot]))

    def start(s):
        for copy in cache_copies(s):
            copy.start()

    def wait(s):
        for copy in cache_copies(s):
            copy.wait()

    for copy in weights[:4]:
        copy.start()

    lane128 = lax.broadcasted_iota(jnp.int32, (1, 128), 1)
    lane256 = lax.broadcasted_iota(jnp.int32, (1, 256), 1)

    dot = functools.partial(jnp.dot, preferred_element_type=F32)
    dot_t = functools.partial(lax.dot_general, dimension_numbers=(((1,), (1,)), ((), ())), preferred_element_type=F32)

    def fill(b, _):
        ctxv[pl.ds(b, 1), :] = jnp.full((1, 128), ctx_ref[b], jnp.int32)
        return 0
    lax.fori_loop(0, NREQ, fill, 0)
    angle = ctxv[...].astype(F32) * freq_ref[...]
    cos_t = jnp.cos(angle)
    sin_t = jnp.sin(angle) * jnp.where(lax.rem(lane128, 32) < 16, -1.0, 1.0)

    weights[0].wait()
    cq = [dot(x_ref[...], wdq[:, n * 256:(n + 1) * 256]).astype(BF16).astype(F32) for n in range(3)]
    mean_sq = sum(jnp.sum(v * v, axis=1, keepdims=True) for v in cq) * np.float32(1.0 / QL)
    inv_q = lax.rsqrt(mean_sq + NORM_EPS)
    cn = jnp.concatenate([(cq[n] * inv_q * gq_ref[n * 256:(n + 1) * 256][None, :]).astype(BF16) for n in range(3)], axis=1)

    weights[1].wait()
    kv = dot_t(x_ref[...], wdkv[:L, :])
    inv_kv = lax.rsqrt(jnp.sum(kv * kv, axis=1, keepdims=True) * np.float32(1.0 / L) + NORM_EPS)
    c_new = (kv * inv_kv * gkv_ref[...][None, :]).astype(BF16)
    co_ref[...] = c_new
    cnf[...] = c_new.astype(F32)
    kr = dot_t(x_ref[...], wdkv[L:L + R, :])
    kr = jnp.concatenate([kr, jnp.zeros((NREQ, 128 - R), F32)], axis=1)
    partner = jnp.where(lane128 < 16, pltpu.roll(kr, 112, 1), pltpu.roll(kr, 16, 1))
    kr_new = (kr * cos_t + partner * sin_t).astype(BF16)
    ko_ref[...] = jnp.where(lane128 < R, kr_new, jnp.zeros_like(kr_new))
    krf[...] = jnp.where(lane128 < R, kr_new.astype(F32), 0.0)

    weights[2].wait()
    for s in range(NB):
        start(s)
    for n in range(15):
        qf[:, n * 256:(n + 1) * 256] = dot(cn, wuq[:, n * 256:(n + 1) * 256]).astype(BF16)

    row = lax.broadcasted_iota(jnp.int32, (256, 256), 0)
    col = lax.broadcasted_iota(jnp.int32, (256, 256), 1)
    src = lax.rem(col + jnp.where(col < 128, 0, 16), 32)
    for o in range(8):
        pick = jnp.where(row == src + 32 * o, 1.0, 0.0).astype(BF16)
        heads = [h for h in range(H) if ((96 * h + 64) % 256) // 32 == o]
        wins = [(96 * h + 64) // 256 for h in heads]
        both = dot(jnp.concatenate([qf[:, w * 256:(w + 1) * 256] for w in wins], axis=0), pick)
        for k, h in enumerate(heads):
            part = both[k * NREQ:(k + 1) * NREQ]
            qrf[pl.ds(h, NREQ, stride=H), :] = (part[:, :128] * cos_t + part[:, 128:] * sin_t).astype(BF16).astype(F32)

    weights[3].wait()
    nope = {h: (96 * h, 96 * h + 64) for h in range(H)}
    carry = {}
    for w in range(15):
        lo, hi = 256 * w, 256 * (w + 1)
        here = [(h, max(a, lo), min(b, hi)) for h, (a, b) in nope.items() if a < hi and b > lo]
        pieces, at = [], lo
        for h, a, b in here:
            if a > at:
                pieces.append(jnp.zeros((a - at, 256), BF16))
            pieces.append(wuk[h, a - nope[h][0]:b - nope[h][0], :])
            at = b
        if at < hi:
            pieces.append(jnp.zeros((hi - at, 256), BF16))
        window = qf[:, lo:hi]
        lhs = [window * jnp.where((lane256 >= a - lo) & (lane256 < b - lo), 1.0, 0.0).astype(BF16) for _, a, b in here]
        lat = dot(jnp.concatenate(lhs, axis=0), jnp.concatenate(pieces, axis=0))
        for k, (h, a, b) in enumerate(here):
            v = lat[k * NREQ:(k + 1) * NREQ]
            if a > nope[h][0]:
                v = v + carry.pop(h)
            if b < nope[h][1]:
                carry[h] = v
                continue
            v = v.astype(BF16).astype(F32)
            qla[pl.ds(h, NREQ, stride=H), :] = v[:, :128]
            qlb[pl.ds(h, NREQ, stride=H), :] = v[:, 128:]
    pl.semaphore_wait(barrier, 2)

    def head_rows(i):
        return pl.ds(pl.multiple_of(i * H, 8), H)

    def rcopy_1(i):
        return pltpu.make_async_remote_copy(src_ref=send_a.at[i], dst_ref=recv_1.at[i], send_sem=sa_sem.at[i], recv_sem=r1_sem.at[i],
                                            device_id={'cp': sibling}, device_id_type=pl.DeviceIdType.MESH)

    def rcopy_2(i):
        return pltpu.make_async_remote_copy(src_ref=send_b.at[i], dst_ref=recv_2.at[i], send_sem=sb_sem.at[i], recv_sem=r2_sem.at[i],
                                            device_id={'cp': mirror}, device_id_type=pl.DeviceIdType.MESH)

    def put_partial(ref, i, lo, hi, m, l):
        ref[i, 0:H, :] = lo
        ref[i, H:2 * H, :] = hi
        ml = jnp.zeros((8, 128), F32)
        for g in range(5):
            ml = jnp.where(lane128 == g, m[8 * g:8 * g + 8], ml)
            ml = jnp.where(lane128 == 8 + g, l[8 * g:8 * g + 8], ml)
        ref[i, 2 * H:2 * H + 8, :] = ml

    def get_partial(ref, i):
        ml = ref[i, 2 * H:2 * H + 8, :]
        spread = lambda at: jnp.concatenate([jnp.broadcast_to(ml[:, at + g:at + g + 1], (8, 128)) for g in range(5)], axis=0)
        return ref[i, 0:H, :], ref[i, H:2 * H, :], spread(0), spread(8)

    def combine_1(i):
        lo_p, hi_p, m_p, l_p = get_partial(own_b, i)
        lo_q, hi_q, m_q, l_q = get_partial(recv_1, i)
        m = jnp.maximum(m_p, m_q)
        f_p, f_q = jnp.exp2(m_p - m), jnp.exp2(m_q - m)
        put_partial(send_b, i, lo_p * f_p + lo_q * f_q, hi_p * f_p + hi_q * f_q, m, l_p * f_p + l_q * f_q)

    def combine_2(i):
        lo_p, hi_p, m_p, l_p = get_partial(send_b, i)
        lo_q, hi_q, m_q, l_q = get_partial(recv_2, i)
        ii = jnp.minimum(i, NOWN - 1)
        b = core * NOWN + ii
        c_row, k_row = cnf[pl.ds(b, 1), :], krf[pl.ds(b, 1), :]
        mine = head_rows(b)
        part = qla[mine, :] * c_row[:, :128] + qlb[mine, :] * c_row[:, 128:] + qrf[mine, :] * k_row
        s_new = jnp.broadcast_to(jnp.sum(part, axis=1, keepdims=True) * SCALE, (H, 128))
        m = jnp.maximum(jnp.maximum(m_p, m_q), s_new)
        f_p, f_q, w_new = jnp.exp2(m_p - m), jnp.exp2(m_q - m), jnp.exp2(s_new - m)
        inv = 1.0 / (l_p * f_p + l_q * f_q + w_new)
        w_new = w_new.astype(BF16).astype(F32)
        rows = head_rows(i)
        ola[rows, :] = (lo_p * f_p + lo_q * f_q + w_new * c_row[:, :128]) * inv
        olb[rows, :] = (hi_p * f_p + hi_q * f_q + w_new * c_row[:, 128:]) * inv

    def attend():
        def load_q(s, par):
            rows = head_rows(request(s))
            q = jnp.concatenate([qla[rows, :], qlb[rows, :]], axis=1)
            qb[par] = jnp.concatenate([q, jnp.zeros((HP - H, L), F32)], axis=0).astype(BF16)
            qrb[par] = jnp.concatenate([qrf[rows, :], jnp.zeros((HP - H, 128), F32)], axis=0).astype(BF16)

        def qk_tile(s, par, j, mx):
            slot, b = lax.rem(s, NB), request(s)
            n = ctx_ref[b] - cp * T
            at = pl.ds(256 * j, 256)
            c = cbuf[slot, at, :]
            if (par, j // 2) in XPOSE_TILES:
                v = dot_t(qb[par], c)
            else:
                v = dot(qb[par], jnp.concatenate([c[:, :128].T, c[:, 128:].T], axis=0))
            v = (v + dot(qrb[par, :, :R], krbuf[slot, :, at]))[:H]
            v = jnp.where(lane256 + j * 256 < n, v, MASKED)
            sbuf[par, :, at] = v
            for k in range(2):
                part = v[:, k * 128:(k + 1) * 128]
                mx = part if mx is None else jnp.maximum(mx, part)
            return mx

        def pv_tile(s, par, j, mk, st):
            ws = []
            for k in range(2):
                w = jnp.exp2(sbuf[par, :, pl.ds(j * 256 + k * 128, 128)] * SCALE - mk)
                st['l'] = w if st['l'] is None else st['l'] + w
                ws.append(w)
            w = jnp.concatenate([jnp.concatenate(ws, axis=1), jnp.zeros((HP - H, 256), F32)], axis=0).astype(BF16)
            p = dot(w, cbuf[lax.rem(s, NB), pl.ds(256 * j, 256), :])
            st[j % 2] = p if st[j % 2] is None else st[j % 2] + p

        def half(s, par, out, out_i, last=False):
            mk = jnp.broadcast_to(jnp.maximum(jnp.max(mbuf[par], axis=1, keepdims=True), FLOOR) * SCALE, (H, 128))
            mx, st = None, {0: None, 1: None, 'l': None}
            if not last:
                load_q(s + 1, 1 - par)
            for j in range(2 * (NT + LEAD)):
                if not last and j < 2 * NT:
                    mx = qk_tile(s + 1, 1 - par, j, mx)
                if j >= 2 * LEAD:
                    pv_tile(s, par, j - 2 * LEAD, mk, st)
            if not last:
                mbuf[1 - par] = mx
            a = (st[0] + st[1])[:H]
            l = jnp.broadcast_to(jnp.sum(st['l'], axis=1, keepdims=True), (H, 128))
            put_partial(out, out_i, a[:, :128], a[:, 128:], mk, l)

        for ref in (own_b, recv_1, send_b, recv_2):
            ref[NOWN] = jnp.zeros((2 * H + 8, 128), F32)

        wait(0)
        load_q(0, 0)
        mx = None
        for j in range(2 * NT):
            mx = qk_tile(0, 0, j, mx)
        mbuf[0] = mx

        def trip(i, last=False):
            s = 2 * i
            wait(s + 1)
            if not last:
                wait(s + 2)

            def when(lag, act):
                if isinstance(i, int):
                    if i >= lag:
                        act()
                else:
                    pl.when(i >= lag)(act)
            when(1, lambda: rcopy_1(i - 1).start())
            when(2, lambda: rcopy_1(i - 2).wait_recv())
            when(3, lambda: rcopy_2(i - 3).start())
            when(6, lambda: rcopy_2(i - 6).wait_recv())
            lagged = lambda lag: jnp.where(i >= lag, i - lag, NOWN)
            half(s, 0, send_a, i)
            combine_1(lagged(2))
            if last:
                rcopy_1(i).start()
                rcopy_1(i - 1).wait_recv()
                combine_1(i - 1)
                rcopy_2(i - 2).start()
            half(s + 1, 1, own_b, i, last=last)
            combine_2(lagged(6))

        def loop_trip(i, _):
            trip(i)
            for u in range(2):
                s = 2 * i + u
                pl.when(s + NB < NREQ)(lambda s=s: start(s + NB))

            @pl.when(i == NREQ // 2 - NB // 2)
            def _():
                for copy in weights[4:]:
                    copy.start()
            return 0
        lax.fori_loop(0, NOWN - 1, loop_trip, 0)
        trip(NOWN - 1, last=True)
        rcopy_1(NOWN - 1).wait_recv()
        rcopy_2(NOWN - 2).start()
        combine_1(NOWN - 1)
        for i in range(NOWN - 6, NOWN):
            rcopy_2(i).wait_recv()
            combine_2(i)
            if i == NOWN - 6:
                rcopy_2(NOWN - 1).start()

    attend()

    def output():
        weights[4].wait()
        groups = []
        for g in range(10):
            rhs = jnp.concatenate([wuv[4 * g + k] for k in range(4)], axis=0)
            at = [pl.ds(4 * g + k, NOWN, stride=H) for k in range(4)]
            lhs = jnp.concatenate([jnp.concatenate([ola[r, :], olb[r, :]], axis=1) for r in at], axis=0).astype(BF16)
            v = dot_t(lhs, rhs)
            o = v[3 * NOWN:]
            for k in range(3):
                o = jnp.where(lane256 // 64 == k, v[k * NOWN:(k + 1) * NOWN], o)
            groups.append(o.astype(BF16))
        heads = jnp.concatenate(groups, axis=1)
        weights[5].wait()
        mine = pl.ds(pl.multiple_of(core * NOWN, NOWN), NOWN)

        def xcopy(n):
            piece = xbuf.at[mine, pl.ds(n * 1280, 1280)]
            return pltpu.make_async_remote_copy(src_ref=piece, dst_ref=piece, send_sem=xs_sem.at[n], recv_sem=xr_sem.at[n],
                                                device_id={'cp': sibling}, device_id_type=pl.DeviceIdType.MESH)

        for n in range(2):
            for k in range(5 * n, 5 * n + 5):
                xbuf[mine, k * 256:(k + 1) * 256] = dot(heads, wo[:, k * 256:(k + 1) * 256])
            xcopy(n).start()
        for n in range(2):
            xcopy(n).wait_recv()
        xo_ref[...] = (x_ref[...].astype(F32) + xbuf[...]).astype(BF16)
        for n in range(2):
            xcopy(n).wait_send()

        def sent(i, _):
            rcopy_1(i).wait_send()
            rcopy_2(i).wait_send()
            return 0
        lax.fori_loop(0, NOWN, sent, 0)

    output()


def finish_kernel(x_ref, c_ref, k_ref, xo_ref, co_ref, ko_ref):
    xo_ref[...] = x_ref[...]
    co_ref[...] = c_ref[...]
    ko_ref[...] = k_ref[...].astype(F32).T[:R].astype(BF16)


def solution(mesh):
    half_dim = R // 2
    freq = 10000.0 ** (-2.0 * np.arange(half_dim, dtype=np.float64) / R)
    freq = np.tile(freq.astype(np.float32), 8)[None, :]

    def decode_step(x, w_dq, g_q, w_uq, w_dkv, g_kv, w_uk, w_uv, w_o, cache_c, cache_kr, ctx_len):
        vmem, hbm = pl.BlockSpec(memory_space=pltpu.VMEM), pl.BlockSpec(memory_space=pl.ANY)
        dma = pltpu.SemaphoreType.DMA
        part = pltpu.VMEM((NOWN + 1, 2 * H + 8, 128), F32)
        call = pl.pallas_call(
            decode_kernel,
            out_shape=(jax.ShapeDtypeStruct((NREQ, D), BF16), jax.ShapeDtypeStruct((NREQ, L), BF16), jax.ShapeDtypeStruct((NREQ, 128), BF16)),
            in_specs=[vmem] * 4 + [pl.BlockSpec(memory_space=pltpu.SMEM)] + [hbm] * 8,
            out_specs=[vmem] * 3,
            scratch_shapes=[
                pltpu.VMEM((D, QL), BF16), pltpu.VMEM((QL, H * 96), BF16), pltpu.VMEM((L + R, D), BF16),
                pltpu.VMEM((H, 64, L), BF16), pltpu.VMEM((H, 64, L), BF16), pltpu.VMEM((H * 64, D), BF16),
                pltpu.VMEM((NB, T, L), BF16), pltpu.VMEM((NB, R, T), BF16),
                pltpu.VMEM((NREQ, H * 96), BF16), pltpu.VMEM((NREQ * H, 128), F32), pltpu.VMEM((NREQ * H, 128), F32), pltpu.VMEM((NREQ * H, 128), F32),
                pltpu.VMEM((2, HP, L), BF16), pltpu.VMEM((2, HP, 128), BF16),
                pltpu.VMEM((NREQ, L), F32), pltpu.VMEM((NREQ, 128), F32), pltpu.VMEM((NREQ, 128), jnp.int32),
                pltpu.VMEM((2, H, T), F32), pltpu.VMEM((2, H, 128), F32),
                part, part, part, part, part,
                pltpu.VMEM(((NOWN + 1) * H, 128), F32), pltpu.VMEM(((NOWN + 1) * H, 128), F32), pltpu.VMEM((NREQ, D), F32),
                dma((6,)), dma((NB,)), dma((NB,)), dma((NOWN,)), dma((NOWN,)), dma((NOWN,)), dma((NOWN,)), dma((10,)), dma((10,)),
            ],
            compiler_params=pltpu.CompilerParams(collective_id=0, has_side_effects=True, vmem_limit_bytes=67_043_328),
        )
        outs = call(x, g_q, g_kv, jnp.asarray(freq), ctx_len, w_dq, w_uq, w_dkv.T,
                    jnp.transpose(w_uk, (1, 2, 0)), jnp.transpose(w_uv, (1, 2, 0)), w_o, cache_c, jnp.swapaxes(cache_kr, 1, 2))
        shapes = [jax.ShapeDtypeStruct(shape, BF16) for shape in ((NREQ, D), (NREQ, L), (R, NREQ))]
        x_out, c_new, kr_new = pl.pallas_call(finish_kernel, out_shape=shapes, in_specs=[vmem] * 3, out_specs=[vmem] * 3)(*outs)
        return x_out, c_new, kr_new.T

    rows, cache = P('dp', None), P('dp', 'cp', None)
    in_specs = (rows, P(), P(), P(), P(), P(), P(), P(), P(), cache, cache, P('dp'))
    return jax.shard_map(decode_step, mesh=mesh, in_specs=in_specs, out_specs=(rows, rows, rows), check_vma=False)
```

```python
import functools

import jax
import jax.numpy as jnp
import numpy as np
from jax import lax
from jax.experimental import pallas as pl
from jax.experimental.pallas import tpu as pltpu
from jax.sharding import PartitionSpec as P

F32, BF16 = jnp.float32, jnp.bfloat16
NORM_EPS = 1e-6
SCALE = np.float32(96 ** -0.5 * np.log2(np.e))
MASKED = -2.0e38
FLOOR = -1.0e38

NREQ, T, H, L, R, D, QL = 64, 4096, 40, 256, 32, 2560, 768
HP = 48
NT = 8
NB = 8
NOWN = NREQ // 2
LEAD = 4
XPOSE_TILES = ((1, 0), (0, 1))


def decode_kernel(x_ref, gq_ref, gkv_ref, freq_ref, ctx_ref, wdq_h, wuq_h, wdkv_h, wuk_h, wuv_h, wo_h, c_h, kr_h,
                  xo_ref, co_ref, ko_ref,
                  wdq, wuq, wdkv, wuk, wuv, wo, cbuf, krbuf, qf, qla, qlb, qrf, qb, qrb, cnf, krf, ctxv,
                  sbuf, mbuf, send_a, recv_1, own_b, send_b, recv_2, ola, olb, xbuf,
                  wsem, csem, ksem, sa_sem, r1_sem, sb_sem, r2_sem, xs_sem, xr_sem):
    cp = lax.axis_index('cp')
    core = lax.rem(cp, 2)
    sibling = cp + 1 - 2 * core
    mirror = lax.rem(cp + 2, 4)

    barrier = pltpu.get_barrier_semaphore()
    for other in (sibling, mirror):
        pl.semaphore_signal(barrier, inc=1, device_id={'cp': other}, device_id_type=pl.DeviceIdType.MESH)

    weights = [pltpu.make_async_copy(h, v, wsem.at[k]) for k, (h, v) in enumerate(
        ((wdq_h, wdq), (wdkv_h, wdkv), (wuq_h, wuq), (wuk_h, wuk), (wuv_h, wuv), (wo_h, wo)))]

    def request(s):
        u = lax.rem(s, 2)
        half = (1 - core) * (1 - u) + core * u
        return half * NOWN + s // 2

    def cache_copies(s):
        b, slot = request(s), lax.rem(s, NB)
        return (pltpu.make_async_copy(c_h.at[b], cbuf.at[slot], csem.at[slot]),
                pltpu.make_async_copy(kr_h.at[b], krbuf.at[slot], ksem.at[slot]))

    def start(s):
        for copy in cache_copies(s):
            copy.start()

    def wait(s):
        for copy in cache_copies(s):
            copy.wait()

    for copy in weights[:4]:
        copy.start()

    lane128 = lax.broadcasted_iota(jnp.int32, (1, 128), 1)
    lane256 = lax.broadcasted_iota(jnp.int32, (1, 256), 1)

    dot = functools.partial(jnp.dot, preferred_element_type=F32)
    dot_t = functools.partial(lax.dot_general, dimension_numbers=(((1,), (1,)), ((), ())), preferred_element_type=F32)

    def fill(b, _):
        ctxv[pl.ds(b, 1), :] = jnp.full((1, 128), ctx_ref[b], jnp.int32)
        return 0
    lax.fori_loop(0, NREQ, fill, 0)
    angle = ctxv[...].astype(F32) * freq_ref[...]
    cos_t = jnp.cos(angle)
    sin_t = jnp.sin(angle) * jnp.where(lax.rem(lane128, 32) < 16, -1.0, 1.0)

    weights[0].wait()
    cq = [dot(x_ref[...], wdq[:, n * 256:(n + 1) * 256]).astype(BF16).astype(F32) for n in range(3)]
    mean_sq = sum(jnp.sum(v * v, axis=1, keepdims=True) for v in cq) * np.float32(1.0 / QL)
    inv_q = lax.rsqrt(mean_sq + NORM_EPS)
    cn = jnp.concatenate([(cq[n] * inv_q * gq_ref[n * 256:(n + 1) * 256][None, :]).astype(BF16) for n in range(3)], axis=1)

    weights[1].wait()
    kv = dot_t(x_ref[...], wdkv[:L, :])
    inv_kv = lax.rsqrt(jnp.sum(kv * kv, axis=1, keepdims=True) * np.float32(1.0 / L) + NORM_EPS)
    c_new = (kv * inv_kv * gkv_ref[...][None, :]).astype(BF16)
    co_ref[...] = c_new
    cnf[...] = c_new.astype(F32)
    kr = dot_t(x_ref[...], wdkv[L:L + R, :])
    kr = jnp.concatenate([kr, jnp.zeros((NREQ, 128 - R), F32)], axis=1)
    partner = jnp.where(lane128 < 16, pltpu.roll(kr, 112, 1), pltpu.roll(kr, 16, 1))
    kr_new = (kr * cos_t + partner * sin_t).astype(BF16)
    ko_ref[...] = jnp.where(lane128 < R, kr_new, jnp.zeros_like(kr_new))
    krf[...] = jnp.where(lane128 < R, kr_new.astype(F32), 0.0)

    weights[2].wait()
    for s in range(NB):
        start(s)
    for n in range(15):
        qf[:, n * 256:(n + 1) * 256] = dot(cn, wuq[:, n * 256:(n + 1) * 256]).astype(BF16)

    row = lax.broadcasted_iota(jnp.int32, (256, 256), 0)
    col = lax.broadcasted_iota(jnp.int32, (256, 256), 1)
    src = lax.rem(col + jnp.where(col < 128, 0, 16), 32)
    for o in range(8):
        pick = jnp.where(row == src + 32 * o, 1.0, 0.0).astype(BF16)
        heads = [h for h in range(H) if ((96 * h + 64) % 256) // 32 == o]
        wins = [(96 * h + 64) // 256 for h in heads]
        both = dot(jnp.concatenate([qf[:, w * 256:(w + 1) * 256] for w in wins], axis=0), pick)
        for k, h in enumerate(heads):
            part = both[k * NREQ:(k + 1) * NREQ]
            qrf[pl.ds(h, NREQ, stride=H), :] = (part[:, :128] * cos_t + part[:, 128:] * sin_t).astype(BF16).astype(F32)

    weights[3].wait()
    nope = {h: (96 * h, 96 * h + 64) for h in range(H)}
    carry = {}
    for w in range(15):
        lo, hi = 256 * w, 256 * (w + 1)
        here = [(h, max(a, lo), min(b, hi)) for h, (a, b) in nope.items() if a < hi and b > lo]
        pieces, at = [], lo
        for h, a, b in here:
            if a > at:
                pieces.append(jnp.zeros((a - at, 256), BF16))
            pieces.append(wuk[h, a - nope[h][0]:b - nope[h][0], :])
            at = b
        if at < hi:
            pieces.append(jnp.zeros((hi - at, 256), BF16))
        window = qf[:, lo:hi]
        lhs = [window * jnp.where((lane256 >= a - lo) & (lane256 < b - lo), 1.0, 0.0).astype(BF16) for _, a, b in here]
        lat = dot(jnp.concatenate(lhs, axis=0), jnp.concatenate(pieces, axis=0))
        for k, (h, a, b) in enumerate(here):
            v = lat[k * NREQ:(k + 1) * NREQ]
            if a > nope[h][0]:
                v = v + carry.pop(h)
            if b < nope[h][1]:
                carry[h] = v
                continue
            v = v.astype(BF16).astype(F32)
            qla[pl.ds(h, NREQ, stride=H), :] = v[:, :128]
            qlb[pl.ds(h, NREQ, stride=H), :] = v[:, 128:]
    pl.semaphore_wait(barrier, 2)

    def head_rows(i):
        return pl.ds(pl.multiple_of(i * H, 8), H)

    def rcopy_1(i):
        return pltpu.make_async_remote_copy(src_ref=send_a.at[i], dst_ref=recv_1.at[i], send_sem=sa_sem.at[i], recv_sem=r1_sem.at[i],
                                            device_id={'cp': sibling}, device_id_type=pl.DeviceIdType.MESH)

    def rcopy_2(i):
        return pltpu.make_async_remote_copy(src_ref=send_b.at[i], dst_ref=recv_2.at[i], send_sem=sb_sem.at[i], recv_sem=r2_sem.at[i],
                                            device_id={'cp': mirror}, device_id_type=pl.DeviceIdType.MESH)

    def put_partial(ref, i, lo, hi, m, l):
        ref[i, 0:H, :] = lo
        ref[i, H:2 * H, :] = hi
        ml = jnp.zeros((8, 128), F32)
        for g in range(5):
            ml = jnp.where(lane128 == g, m[8 * g:8 * g + 8], ml)
            ml = jnp.where(lane128 == 8 + g, l[8 * g:8 * g + 8], ml)
        ref[i, 2 * H:2 * H + 8, :] = ml

    def get_partial(ref, i):
        ml = ref[i, 2 * H:2 * H + 8, :]
        spread = lambda at: jnp.concatenate([jnp.broadcast_to(ml[:, at + g:at + g + 1], (8, 128)) for g in range(5)], axis=0)
        return ref[i, 0:H, :], ref[i, H:2 * H, :], spread(0), spread(8)

    def combine_1(i):
        lo_p, hi_p, m_p, l_p = get_partial(own_b, i)
        lo_q, hi_q, m_q, l_q = get_partial(recv_1, i)
        m = jnp.maximum(m_p, m_q)
        f_p, f_q = jnp.exp2(m_p - m), jnp.exp2(m_q - m)
        put_partial(send_b, i, lo_p * f_p + lo_q * f_q, hi_p * f_p + hi_q * f_q, m, l_p * f_p + l_q * f_q)

    def combine_2(i):
        lo_p, hi_p, m_p, l_p = get_partial(send_b, i)
        lo_q, hi_q, m_q, l_q = get_partial(recv_2, i)
        ii = jnp.minimum(i, NOWN - 1)
        b = core * NOWN + ii
        c_row, k_row = cnf[pl.ds(b, 1), :], krf[pl.ds(b, 1), :]
        mine = head_rows(b)
        part = qla[mine, :] * c_row[:, :128] + qlb[mine, :] * c_row[:, 128:] + qrf[mine, :] * k_row
        s_new = jnp.broadcast_to(jnp.sum(part, axis=1, keepdims=True) * SCALE, (H, 128))
        m = jnp.maximum(jnp.maximum(m_p, m_q), s_new)
        f_p, f_q, w_new = jnp.exp2(m_p - m), jnp.exp2(m_q - m), jnp.exp2(s_new - m)
        inv = 1.0 / (l_p * f_p + l_q * f_q + w_new)
        w_new = w_new.astype(BF16).astype(F32)
        rows = head_rows(i)
        ola[rows, :] = (lo_p * f_p + lo_q * f_q + w_new * c_row[:, :128]) * inv
        olb[rows, :] = (hi_p * f_p + hi_q * f_q + w_new * c_row[:, 128:]) * inv

    def attend():
        def load_q(s, par):
            rows = head_rows(request(s))
            q = jnp.concatenate([qla[rows, :], qlb[rows, :]], axis=1)
            qb[par] = jnp.concatenate([q, jnp.zeros((HP - H, L), F32)], axis=0).astype(BF16)
            qrb[par] = jnp.concatenate([qrf[rows, :], jnp.zeros((HP - H, 128), F32)], axis=0).astype(BF16)

        def qk_tile(s, par, j, mx):
            slot, b = lax.rem(s, NB), request(s)
            n = ctx_ref[b] - cp * T
            at = pl.ds(256 * j, 256)
            c = cbuf[slot, at, :]
            if (par, j // 2) in XPOSE_TILES:
                v = dot_t(qb[par], c)
            else:
                v = dot(qb[par], jnp.concatenate([c[:, :128].T, c[:, 128:].T], axis=0))
            v = (v + dot(qrb[par, :, :R], krbuf[slot, :, at]))[:H]
            v = jnp.where(lane256 + j * 256 < n, v, MASKED)
            sbuf[par, :, at] = v
            for k in range(2):
                part = v[:, k * 128:(k + 1) * 128]
                mx = part if mx is None else jnp.maximum(mx, part)
            return mx

        def pv_tile(s, par, j, mk, st):
            ws = []
            for k in range(2):
                w = jnp.exp2(sbuf[par, :, pl.ds(j * 256 + k * 128, 128)] * SCALE - mk)
                st['l'] = w if st['l'] is None else st['l'] + w
                ws.append(w)
            w = jnp.concatenate([jnp.concatenate(ws, axis=1), jnp.zeros((HP - H, 256), F32)], axis=0).astype(BF16)
            p = dot(w, cbuf[lax.rem(s, NB), pl.ds(256 * j, 256), :])
            st[j % 2] = p if st[j % 2] is None else st[j % 2] + p

        def half(s, par, out, out_i, last=False):
            mk = jnp.broadcast_to(jnp.maximum(jnp.max(mbuf[par], axis=1, keepdims=True), FLOOR) * SCALE, (H, 128))
            mx, st = None, {0: None, 1: None, 'l': None}
            if not last:
                load_q(s + 1, 1 - par)
            for j in range(2 * (NT + LEAD)):
                if not last and j < 2 * NT:
                    mx = qk_tile(s + 1, 1 - par, j, mx)
                if j >= 2 * LEAD:
                    pv_tile(s, par, j - 2 * LEAD, mk, st)
            if not last:
                mbuf[1 - par] = mx
            a = (st[0] + st[1])[:H]
            l = jnp.broadcast_to(jnp.sum(st['l'], axis=1, keepdims=True), (H, 128))
            put_partial(out, out_i, a[:, :128], a[:, 128:], mk, l)

        for ref in (own_b, recv_1, send_b, recv_2):
            ref[NOWN] = jnp.zeros((2 * H + 8, 128), F32)

        wait(0)
        load_q(0, 0)
        mx = None
        for j in range(2 * NT):
            mx = qk_tile(0, 0, j, mx)
        mbuf[0] = mx

        def trip(i, last=False):
            s = 2 * i
            wait(s + 1)
            if not last:
                wait(s + 2)

            def when(lag, act):
                if isinstance(i, int):
                    if i >= lag:
                        act()
                else:
                    pl.when(i >= lag)(act)
            when(1, lambda: rcopy_1(i - 1).start())
            when(2, lambda: rcopy_1(i - 2).wait_recv())
            when(3, lambda: rcopy_2(i - 3).start())
            when(6, lambda: rcopy_2(i - 6).wait_recv())
            lagged = lambda lag: jnp.where(i >= lag, i - lag, NOWN)
            half(s, 0, send_a, i)
            combine_1(lagged(2))
            if last:
                rcopy_1(i).start()
                rcopy_1(i - 1).wait_recv()
                combine_1(i - 1)
                rcopy_2(i - 2).start()
            half(s + 1, 1, own_b, i, last=last)
            combine_2(lagged(6))

        def loop_trip(i, _):
            trip(i)
            for u in range(2):
                s = 2 * i + u
                pl.when(s + NB < NREQ)(lambda s=s: start(s + NB))

            @pl.when(i == NREQ // 2 - NB // 2)
            def _():
                for copy in weights[4:]:
                    copy.start()
            return 0
        lax.fori_loop(0, NOWN - 1, loop_trip, 0)
        trip(NOWN - 1, last=True)
        rcopy_1(NOWN - 1).wait_recv()
        rcopy_2(NOWN - 2).start()
        combine_1(NOWN - 1)
        for i in range(NOWN - 6, NOWN):
            rcopy_2(i).wait_recv()
            combine_2(i)
            if i == NOWN - 6:
                rcopy_2(NOWN - 1).start()

    attend()

    def output():
        weights[4].wait()
        groups = []
        for g in range(10):
            rhs = jnp.concatenate([wuv[4 * g + k] for k in range(4)], axis=0)
            at = [pl.ds(4 * g + k, NOWN, stride=H) for k in range(4)]
            lhs = jnp.concatenate([jnp.concatenate([ola[r, :], olb[r, :]], axis=1) for r in at], axis=0).astype(BF16)
            v = dot_t(lhs, rhs)
            o = v[3 * NOWN:]
            for k in range(3):
                o = jnp.where(lane256 // 64 == k, v[k * NOWN:(k + 1) * NOWN], o)
            groups.append(o.astype(BF16))
        heads = jnp.concatenate(groups, axis=1)
        weights[5].wait()
        mine = pl.ds(pl.multiple_of(core * NOWN, NOWN), NOWN)

        def xcopy(n):
            piece = xbuf.at[mine, pl.ds(n * 1280, 1280)]
            return pltpu.make_async_remote_copy(src_ref=piece, dst_ref=piece, send_sem=xs_sem.at[n], recv_sem=xr_sem.at[n],
                                                device_id={'cp': sibling}, device_id_type=pl.DeviceIdType.MESH)

        for n in range(2):
            for k in range(5 * n, 5 * n + 5):
                xbuf[mine, k * 256:(k + 1) * 256] = dot(heads, wo[:, k * 256:(k + 1) * 256])
            xcopy(n).start()
        for n in range(2):
            xcopy(n).wait_recv()
        xo_ref[...] = (x_ref[...].astype(F32) + xbuf[...]).astype(BF16)
        for n in range(2):
            xcopy(n).wait_send()

        def sent(i, _):
            rcopy_1(i).wait_send()
            rcopy_2(i).wait_send()
            return 0
        lax.fori_loop(0, NOWN, sent, 0)

    output()


def finish_kernel(x_ref, c_ref, k_ref, xo_ref, co_ref, ko_ref):
    xo_ref[...] = x_ref[...]
    co_ref[...] = c_ref[...]
    ko_ref[...] = k_ref[...].astype(F32).T[:R].astype(BF16)


def solution(mesh):
    half_dim = R // 2
    freq = 10000.0 ** (-2.0 * np.arange(half_dim, dtype=np.float64) / R)
    freq = np.tile(freq.astype(np.float32), 8)[None, :]

    def decode_step(x, w_dq, g_q, w_uq, w_dkv, g_kv, w_uk, w_uv, w_o, cache_c, cache_kr, ctx_len):
        vmem, hbm = pl.BlockSpec(memory_space=pltpu.VMEM), pl.BlockSpec(memory_space=pl.ANY)
        dma = pltpu.SemaphoreType.DMA
        part = pltpu.VMEM((NOWN + 1, 2 * H + 8, 128), F32)
        call = pl.pallas_call(
            decode_kernel,
            out_shape=(jax.ShapeDtypeStruct((NREQ, D), BF16), jax.ShapeDtypeStruct((NREQ, L), BF16), jax.ShapeDtypeStruct((NREQ, 128), BF16)),
            in_specs=[vmem] * 4 + [pl.BlockSpec(memory_space=pltpu.SMEM)] + [hbm] * 8,
            out_specs=[vmem] * 3,
            scratch_shapes=[
                pltpu.VMEM((D, QL), BF16), pltpu.VMEM((QL, H * 96), BF16), pltpu.VMEM((L + R, D), BF16),
                pltpu.VMEM((H, 64, L), BF16), pltpu.VMEM((H, 64, L), BF16), pltpu.VMEM((H * 64, D), BF16),
                pltpu.VMEM((NB, T, L), BF16), pltpu.VMEM((NB, R, T), BF16),
                pltpu.VMEM((NREQ, H * 96), BF16), pltpu.VMEM((NREQ * H, 128), F32), pltpu.VMEM((NREQ * H, 128), F32), pltpu.VMEM((NREQ * H, 128), F32),
                pltpu.VMEM((2, HP, L), BF16), pltpu.VMEM((2, HP, 128), BF16),
                pltpu.VMEM((NREQ, L), F32), pltpu.VMEM((NREQ, 128), F32), pltpu.VMEM((NREQ, 128), jnp.int32),
                pltpu.VMEM((2, H, T), F32), pltpu.VMEM((2, H, 128), F32),
                part, part, part, part, part,
                pltpu.VMEM(((NOWN + 1) * H, 128), F32), pltpu.VMEM(((NOWN + 1) * H, 128), F32), pltpu.VMEM((NREQ, D), F32),
                dma((6,)), dma((NB,)), dma((NB,)), dma((NOWN,)), dma((NOWN,)), dma((NOWN,)), dma((NOWN,)), dma((10,)), dma((10,)),
            ],
            compiler_params=pltpu.CompilerParams(collective_id=0, has_side_effects=True, vmem_limit_bytes=67_043_328),
        )
        outs = call(x, g_q, g_kv, jnp.asarray(freq), ctx_len, w_dq, w_uq, w_dkv.T,
                    jnp.transpose(w_uk, (1, 2, 0)), jnp.transpose(w_uv, (1, 2, 0)), w_o, cache_c, jnp.swapaxes(cache_kr, 1, 2))
        shapes = [jax.ShapeDtypeStruct(shape, BF16) for shape in ((NREQ, D), (NREQ, L), (R, NREQ))]
        x_out, c_new, kr_new = pl.pallas_call(finish_kernel, out_shape=shapes, in_specs=[vmem] * 3, out_specs=[vmem] * 3)(*outs)
        return x_out, c_new, kr_new.T

    rows, cache = P('dp', None), P('dp', 'cp', None)
    in_specs = (rows, P(), P(), P(), P(), P(), P(), P(), P(), cache, cache, P('dp'))
    return jax.shard_map(decode_step, mesh=mesh, in_specs=in_specs, out_specs=(rows, rows, rows), check_vma=False)
```
